512 devices in a mesh: facet: 16 (over x_hi, z), col: 32 (over y, x_lo, core).
Axes of the slice: x: 4 (x_hi: 2, x_lo: 2; x = x_hi * 2 + x_lo), y: 8, z: 8, core: 2. Of those that a mesh axis runs over, the one named last changes fastest.
Arguments:
- facets: bfloat16 [16, 256, 2, 128], P('facet', 'col'), may hold values from -6 to 6
- sub_offsets: int32 [32, 16], P('col'), may hold values from 0 to 8191
- col_offsets: int32 [32], P('col'), may hold values from 0 to 8191
- screen_index: int32 [32, 16], P('col', 'facet'), may hold values from 0 to 3
- screens: float32 [4, 2, 256, 256], replicated, may hold values from -6 to 6
Outputs:
- facets_out: float32 [16, 256, 2, 128], P('facet', 'col')
The draws below stay inside these ranges and needn't reach their ends.
All inputs are finite; a program needn't handle non-finite values.
Results may differ from the reference program's by a relative error of at most 0.0056.
Values may be sent and summed in bfloat16 or wider, within the bound.
A program may use at most 64 MiB of HBM per device.

```python
import math
import jax
import jax.numpy as jnp
from jax import lax

XC = 64
XS = 256
SLAB = 128
NPAD = 8192
NSCREEN = 4
NFACET = 16
NCOL = 32
FH = 256
NSUB = 16


def touch_ends(values, own_key, smallest, high):
    place = [jax.random.randint(jax.random.fold_in(own_key, axis), (), 0, length) for axis, length in enumerate(values.shape)]
    main_axis = values.shape.index(max(values.shape))
    beside = place[:main_axis] + [(place[main_axis] + 1) % values.shape[main_axis]] + place[main_axis + 1:]
    return values.at[tuple(place)].set(smallest).at[tuple(beside)].set(high)


def shard_levels(rng, extent, split, smallest, high):
    loudness = 1.0
    for dim, blocks in split:
        draws = jax.random.uniform(jax.random.fold_in(jax.random.fold_in(rng, 6), dim), (blocks,), jnp.float32, smallest / len(split), high / len(split))
        loudness = loudness * jnp.repeat(jnp.exp(draws), extent[dim] // blocks).reshape((-1,) + (1,) * (len(extent) - 1 - dim))
    return loudness


def bell_draw(rng, dims, width, most, shards=(), kind=jnp.bfloat16):
    drawn = jax.random.normal(rng, dims, jnp.float32) * width
    if len(shards) > 0:
        drawn = shard_levels(rng, dims, shards, -0.22, 0.18) * drawn
    return jnp.clip(drawn, min=-most, max=most).astype(kind)


def setup_inputs(seed: int = 0) -> dict:
    keys = jax.random.split(jax.random.key(seed), 6)
    return {
        "facets": bell_draw(keys[0], (NFACET, FH, 2, SLAB), 1.0, 6.0, ((0, 16), (1, 32))),
        "sub_offsets": touch_ends(jax.random.randint(keys[1], (NCOL, NSUB), 0, NPAD), jax.random.fold_in(keys[1], 1), 0, NPAD - 1).astype(jnp.int32),
        "col_offsets": touch_ends(jax.random.randint(keys[2], (NCOL,), 0, NPAD), jax.random.fold_in(keys[2], 1), 0, NPAD - 1).astype(jnp.int32),
        "screen_index": touch_ends(jax.random.randint(keys[3], (NCOL, NSUB), 0, NSCREEN), jax.random.fold_in(keys[3], 1), 0, NSCREEN - 1).astype(jnp.int32),
        "screens": bell_draw(keys[4], (NSCREEN, 2, XS, XS), 1.0, 6.0, (), jnp.float32),
    }


def phase_pair(numerator, period, direction, factor):
    angles = direction * 2.0 * math.pi / period * numerator.astype(jnp.float32)
    return ((jnp.cos(angles) * factor).astype(jnp.bfloat16), (jnp.sin(angles) * factor).astype(jnp.bfloat16))

def embed_table(facet_ids):
    column = jnp.arange(XS, dtype=jnp.int32)
    within = jnp.arange(XC, dtype=jnp.int32)
    product = column[None, :, None] * (within[None, None, :] + 7 * facet_ids[:, None, None]) % XS
    return phase_pair(product, XS, 1.0, 1.0 / math.sqrt(XS))

def column_table(offset):
    position = jnp.arange(SLAB, dtype=jnp.int32)
    frequency = (offset + jnp.arange(XC, dtype=jnp.int32)) % NPAD
    product = position[:, None] * frequency[None, :] % NPAD
    return phase_pair(product, NPAD, -1.0, 1.0 / math.sqrt(SLAB))

def row_table(offsets, row_ids, height):
    frequency = (offsets[:, None] + jnp.arange(XC, dtype=jnp.int32)[None, :]) % NPAD
    frequency = frequency.reshape(frequency.shape + (1,) * row_ids.ndim)
    product = frequency * (row_ids % NPAD) % NPAD
    return phase_pair(product, NPAD, -1.0, 1.0 / math.sqrt(height))

def complex_einsum(form, first_op, second_op):
    first_real = first_op[0].astype(jnp.float32)
    first_imag = first_op[1].astype(jnp.float32)
    second_real = second_op[0].astype(jnp.float32)
    second_imag = second_op[1].astype(jnp.float32)
    real_part = jnp.einsum(form, first_real, second_real) - jnp.einsum(form, first_imag, second_imag)
    imag_part = jnp.einsum(form, first_real, second_imag) + jnp.einsum(form, first_imag, second_real)
    return (real_part, imag_part)

def round_pair(values):
    return (values[0].astype(jnp.bfloat16), values[1].astype(jnp.bfloat16))

def conjugate(values):
    return (values[0], -values[1])

def reference(facets, sub_offsets, col_offsets, screen_index, screens):
    facet_ids = jnp.arange(NFACET, dtype=jnp.int32)
    embedding = embed_table(facet_ids)
    adjoint_embed = conjugate(embedding)
    row_ids = facet_ids[:, None] * FH + jnp.arange(FH, dtype=jnp.int32)[None, :]
    facet_data = (facets[:, :, 0, :], facets[:, :, 1, :])

    def column_step(running, inputs):
        offsets, offset, screen_now = inputs
        across = column_table(offset)
        row_phase = row_table(offsets, row_ids, FH)
        spread = round_pair(complex_einsum('frx,xv->frv', facet_data, across))
        contributions = round_pair(complex_einsum('sufr,frv->fsuv', row_phase, spread))
        halfway = round_pair(complex_einsum('fsuv,fav->fsua', contributions, embedding))
        subgrid = complex_einsum('fau,fsub->sab', embedding, halfway)
        factor = 1.0 / math.sqrt(NFACET)
        sub_real = subgrid[0] * factor
        sub_imag = subgrid[1] * factor
        gain_maps = screens[screen_now]
        gain_real = gain_maps[:, 0]
        gain_imag = gain_maps[:, 1]
        screened = round_pair((sub_real * gain_real - sub_imag * gain_imag, sub_real * gain_imag + sub_imag * gain_real))
        inner = round_pair(complex_einsum('fau,sab->fsub', adjoint_embed, screened))
        returned = round_pair(complex_einsum('fsub,fbv->fsuv', inner, adjoint_embed))
        slab_rows = round_pair(complex_einsum('sufr,fsuv->frv', conjugate(row_phase), returned))
        summand = complex_einsum('frv,xv->frx', slab_rows, conjugate(across))
        return ((running[0] + summand[0], running[1] + summand[1]), None)
    empty_sum = jnp.zeros((NFACET, FH, SLAB), jnp.float32)
    running, _ = lax.scan(column_step, (empty_sum, empty_sum), (sub_offsets, col_offsets, screen_index))
    factor = 1.0 / math.sqrt(NCOL * NSUB)
    return jnp.stack([running[0] * factor, running[1] * factor], axis=2)
```

```python
import functools
import math

import jax
import jax.numpy as jnp
import numpy as np
from jax import lax
from jax.experimental import pallas as pl
from jax.experimental.pallas import tpu as pltpu
from jax.sharding import PartitionSpec as P

XC = 64
XS = 256
SLAB = 128
NPAD = 8192
STEP = 7
ROWS = 8
SPAN = 176
MESH = pl.DeviceIdType.MESH
F32 = jnp.float32
BF16 = jnp.bfloat16


def fourier_tables(facets):
    a = np.arange(XS)[:, None]
    q = np.arange(XS)[None, :]
    angle = 2.0 * np.pi * ((a * q) % XS) / XS
    keep = (q < STEP * (facets - 1) + XC).astype(np.float64)
    re = np.cos(angle) / math.sqrt(XS) * keep
    im = np.sin(angle) / math.sqrt(XS) * keep
    row_in = np.block([[re.T, im.T], [-im.T, re.T]])
    col_in = np.concatenate([re, im], axis=0) / math.sqrt(facets)
    col_out = np.concatenate([re.T[:SPAN], im.T[:SPAN]], axis=0)
    row_out = np.block([[re, -im], [im, re]])
    return tuple(jnp.asarray(t, dtype=BF16) for t in (row_in, col_in, col_out, row_out))


def unit_circle(n):
    n = n & (NPAD - 1)
    quarter = (n + NPAD // 8) >> 11
    t = (n - (quarter << 11)).astype(F32) * (2.0 * math.pi / NPAD)
    t2 = t * t
    c = 1.0 + t2 * (-1.0 / 2 + t2 * (1.0 / 24 + t2 * (-1.0 / 720 + t2 * (1.0 / 40320))))
    s = t * (1.0 + t2 * (-1.0 / 6 + t2 * (1.0 / 120 + t2 * (-1.0 / 5040 + t2 * (1.0 / 362880)))))
    odd = (quarter & 1) == 1
    cos = jnp.where(odd, s, c)
    sin = jnp.where(odd, c, s)
    cos = jnp.where(((quarter + 1) & 2) == 2, -cos, cos)
    sin = jnp.where((quarter & 2) == 2, -sin, sin)
    return cos, sin


def iota(shape, dim):
    return lax.broadcasted_iota(jnp.int32, shape, dim)


def join_parts(t):
    rows = t.shape[0]
    even = (iota(t.shape, 0) & 1) == 0
    low = iota(t.shape, 1) < XC
    other = jnp.where(even, pltpu.roll(t, rows - 1, 0), pltpu.roll(t, 1, 0))
    other = pltpu.roll(other, XC, 1)
    return jnp.where(even == low, t - other, t + other)


def dot(a, b):
    return jnp.dot(a, b, preferred_element_type=F32)


def kernel(
    nf,
    nc,
    x_hbm,
    sub_hbm,
    col_hbm,
    idx_hbm,
    screens_hbm,
    row_in_hbm,
    col_in_hbm,
    col_out_hbm,
    row_out_hbm,
    out_ref,
    sub_s,
    col_s,
    idx_s,
    screens,
    row_in,
    col_in,
    col_out,
    row_out,
    slab,
    phase,
    phase_t,
    across,
    across_t,
    c_out,
    c_in,
    z,
    half,
    w,
    r_out,
    r_in,
    t_out,
    t_in,
    local_sem,
    slab_send,
    slab_recv,
    c_send,
    c_recv,
    r_send,
    r_recv,
    t_send,
    t_recv,
):
    me_f = lax.axis_index("facet")
    me_c = lax.axis_index("col")
    height = ROWS * nc
    block = 2 * ROWS

    def slab_rows(j):
        return pl.ds(pl.multiple_of(j * block, block), block)

    def sub_rows(s):
        return pl.ds(pl.multiple_of(s * XC, XC), XC)

    local = [
        pltpu.make_async_copy(src, dst, local_sem.at[i])
        for i, (src, dst) in enumerate(
            [
                (x_hbm, slab.at[slab_rows(me_c)]),
                (sub_hbm, sub_s),
                (col_hbm, col_s),
                (idx_hbm, idx_s),
                (screens_hbm, screens),
                (row_in_hbm, row_in),
                (col_in_hbm, col_in),
                (col_out_hbm, col_out),
                (row_out_hbm, row_out),
            ]
        )
    ]
    for copy in local:
        copy.start()

    barrier = pltpu.get_barrier_semaphore()

    def greet(axis, me, peers):
        def one(k, carry):
            pl.semaphore_signal(
                barrier, 1, device_id={axis: lax.rem(me + k, peers)}, device_id_type=MESH
            )
            return carry

        lax.fori_loop(1, peers, one, 0)

    greet("col", me_c, nc)
    greet("facet", me_f, nf)

    for copy in local[1:4]:
        copy.wait()
    offset = col_s[0, 0]
    lane = iota((SLAB, 2 * XC), 1)
    cos, sin = unit_circle(iota((SLAB, 2 * XC), 0) * (offset + (lane & (XC - 1))))
    across[...] = (jnp.where(lane < XC, cos, -sin) * (1.0 / math.sqrt(SLAB))).astype(BF16)
    part = iota((2 * XC, SLAB), 0)
    cos, sin = unit_circle(iota((2 * XC, SLAB), 1) * (offset + (part & (XC - 1))))
    across_t[...] = (jnp.where(part < XC, cos, -sin) * (1.0 / math.sqrt(SLAB))).astype(BF16)

    local[0].wait()
    pl.semaphore_wait(barrier, nc - 1 + nf - 1)

    def remote(src, dst, send, recv, axis, peer):
        return pltpu.make_async_remote_copy(
            src_ref=src,
            dst_ref=dst,
            send_sem=send,
            recv_sem=recv,
            device_id={axis: peer},
            device_id_type=MESH,
        )

    def send_slab(k, carry):
        mine = slab.at[slab_rows(me_c)]
        remote(mine, mine, slab_send, slab_recv, "col", lax.rem(me_c + k, nc)).start()
        return carry

    lax.fori_loop(1, nc, send_slab, 0)

    lane_row = (8, 2 * height)
    place = iota(lane_row, 1)
    row_id = me_f * height + (place >> 1)
    turn = (place & 1) * (NPAD // 4)
    within = iota((XC, 2 * height), 0)
    place_u = iota((XC, 2 * height), 1)
    cos_u, sin_u = unit_circle(within * (me_f * height + (place_u >> 1)))
    cos_u = cos_u.reshape(XC // 8, 8, 2 * height)
    sin_u = sin_u.reshape(XC // 8, 8, 2 * height)

    def fill_phase(s, carry):
        cos_s, sin_s = unit_circle(sub_s[0, s] * row_id - turn)
        scale = 1.0 / math.sqrt(height)
        values = (cos_s * scale)[None] * cos_u - (sin_s * scale)[None] * sin_u
        phase[sub_rows(s), :] = values.reshape(XC, 2 * height).astype(BF16)
        return carry

    lax.fori_loop(0, nf, fill_phase, 0)

    tall = (2 * height, 2 * XC)
    row_t = me_f * height + (iota(tall, 0) >> 1)
    turn_t = (iota(tall, 0) & 1) * (NPAD // 4)
    lane_t = iota(tall, 1)

    def fill_phase_t(t, carry):
        freq = jnp.where(lane_t < XC, sub_s[0, 2 * t], sub_s[0, 2 * t + 1]) + (lane_t & (XC - 1))
        cos_t, _ = unit_circle(freq * row_t - turn_t)
        columns = pl.ds(pl.multiple_of(t * 2 * XC, 2 * XC), 2 * XC)
        phase_t[:, columns] = (cos_t * (1.0 / math.sqrt(height))).astype(BF16)
        return carry

    lax.fori_loop(0, nf // 2, fill_phase_t, 0)
    z[...] = jnp.zeros_like(z)
    half[...] = jnp.zeros_like(half)
    for copy in local[4:]:
        copy.wait()

    others = slab.at[pl.ds(0, (nc - 1) * block)]
    arrival = remote(others, others, slab_send, slab_recv, "col", me_c)
    arrival.wait_send()
    arrival.wait_recv()

    spread = join_parts(dot(slab[...], across[...])).astype(BF16)
    c_out[...] = dot(phase[...], spread).astype(BF16)

    def send_c(k, carry):
        peer = lax.rem(me_f + k, nf)
        remote(
            c_out.at[sub_rows(peer)], c_in.at[sub_rows(me_f)], c_send, c_recv.at[me_f], "facet", peer
        ).start()
        return carry

    lax.fori_loop(1, nf, send_c, 0)
    c_in[sub_rows(me_f), :] = c_out[sub_rows(me_f), :]

    lane_c = iota((XC, 2 * XC), 1)
    for f in range(nf):
        start = STEP * f
        rows = pl.ds(start, XC)

        @pl.when(f != me_f)
        def _():
            slot = c_in.at[pl.ds(f * XC, XC)]
            remote(slot, slot, c_send, c_recv.at[f], "facet", me_f).wait_recv()

        got = c_in[pl.ds(f * XC, XC), :].astype(F32)
        re = pltpu.roll(got, start, 1) if start else got
        im = pltpu.roll(got, (start + XC) % (2 * XC), 1)
        first = (lane_c >= start) & (lane_c < start + XC)
        z[rows, 0:128] += jnp.where(first, re, 0.0)
        z[rows, 256:384] += jnp.where(first, im, 0.0)
        if start + XC > 128:
            second = lane_c < start + XC - 128
            z[rows, 128:256] += jnp.where(second, re, 0.0)
            z[rows, 384:512] += jnp.where(second, im, 0.0)

    half[0:SPAN, :] = dot(z[...].astype(BF16), row_in[...]).astype(BF16)
    grid = dot(col_in[...], half[...])
    sub_re = grid[0:XS, 0:XS] - grid[XS:, XS:]
    sub_im = grid[0:XS, XS:] + grid[XS:, 0:XS]
    g = idx_s[0, 0]
    gain_re = screens[g, 0]
    gain_im = screens[g, 1]
    screened = jnp.concatenate(
        [
            (sub_re * gain_re - sub_im * gain_im).astype(BF16),
            (sub_re * gain_im + sub_im * gain_re).astype(BF16),
        ],
        axis=1,
    )
    inner = dot(col_out[...], screened)
    inner = jnp.concatenate(
        [
            (inner[0:SPAN, 0:XS] + inner[SPAN:, XS:]).astype(BF16),
            (inner[0:SPAN, XS:] - inner[SPAN:, 0:XS]).astype(BF16),
        ],
        axis=1,
    )
    w[...] = dot(inner, row_out[...])

    for f in range(nf):
        start = STEP * f
        rows = pl.ds(start, XC)
        re = w[rows, 0:128]
        im = w[rows, 256:384]
        if start + XC > 128:
            re = jnp.where(lane_c >= start, re, w[rows, 128:256])
            im = jnp.where(lane_c >= start, im, w[rows, 384:512])
        re = pltpu.roll(re, 128 - start, 1) if start else re
        im = pltpu.roll(im, (XC + 128 - start) % 128, 1)
        r_out[pl.ds(f * XC, XC), :] = jnp.where(lane_c < XC, re, im).astype(BF16)

    def send_r(k, carry):
        peer = lax.rem(me_f + k, nf)
        remote(
            r_out.at[sub_rows(peer)], r_in.at[sub_rows(me_f)], r_send, r_recv, "facet", peer
        ).start()
        return carry

    lax.fori_loop(1, nf, send_r, 0)
    r_in[sub_rows(me_f), :] = r_out[sub_rows(me_f), :]

    others = r_in.at[pl.ds(0, (nf - 1) * XC)]
    remote(others, others, r_send, r_recv, "facet", me_f).wait_recv()

    rows = join_parts(dot(phase_t[...], r_in[...])).astype(BF16)
    t_out[...] = dot(rows, across_t[...]).astype(BF16)

    def send_t(k, carry):
        peer = lax.rem(me_c + k, nc)
        remote(
            t_out.at[slab_rows(peer)], t_in.at[slab_rows(me_c)], t_send, t_recv, "col", peer
        ).start()
        return carry

    lax.fori_loop(1, nc, send_t, 0)
    t_in[slab_rows(me_c), :] = t_out[slab_rows(me_c), :]

    others = c_in.at[pl.ds(0, (nf - 1) * XC)]
    remote(others, others, c_send, r_recv, "facet", me_f).wait_send()
    remote(others, others, r_send, r_recv, "facet", me_f).wait_send()
    others = t_in.at[pl.ds(0, (nc - 1) * block)]
    arrival = remote(others, others, t_send, t_recv, "col", me_c)
    arrival.wait_send()
    arrival.wait_recv()

    total = jnp.sum(t_in[...].astype(F32).reshape(nc, block, SLAB), axis=0)
    out_ref[...] = total * (1.0 / math.sqrt(nc * nf))


def body(nf, nc, facets, sub_offsets, col_offsets, screen_index, screens):
    block = 2 * ROWS
    height = ROWS * nc
    tables = fourier_tables(nf)
    hbm = pl.BlockSpec(memory_space=pltpu.HBM)
    vmem = pltpu.VMEM
    dma = pltpu.SemaphoreType.DMA
    out = pl.pallas_call(
        functools.partial(kernel, nf, nc),
        name="swiftly",
        out_shape=jax.ShapeDtypeStruct((block, SLAB), F32),
        in_specs=[hbm] * 9,
        out_specs=pl.BlockSpec(memory_space=pltpu.VMEM),
        scratch_shapes=[
            pltpu.SMEM((1, nf), jnp.int32),
            pltpu.SMEM((1, 1), jnp.int32),
            pltpu.SMEM((1, 1), jnp.int32),
            vmem(screens.shape, F32),
            *[vmem(t.shape, BF16) for t in tables],
            vmem((2 * height, SLAB), BF16),
            vmem((nf * XC, 2 * height), BF16),
            vmem((2 * height, nf * XC), BF16),
            vmem((SLAB, 2 * XC), BF16),
            vmem((2 * XC, SLAB), BF16),
            vmem((nf * XC, 2 * XC), BF16),
            vmem((nf * XC, 2 * XC), BF16),
            vmem((SPAN, 2 * XS), F32),
            vmem((XS, 2 * XS), BF16),
            vmem((SPAN, 2 * XS), F32),
            vmem((nf * XC, 2 * XC), BF16),
            vmem((nf * XC, 2 * XC), BF16),
            vmem((2 * height, SLAB), BF16),
            vmem((2 * height, SLAB), BF16),
            dma((9,)),
            dma,
            dma,
            dma,
            dma((nf,)),
            dma,
            dma,
            dma,
            dma,
        ],
        compiler_params=pltpu.CompilerParams(collective_id=0, has_side_effects=True),
    )(
        facets.reshape(block, SLAB),
        sub_offsets,
        col_offsets.reshape(1, 1),
        screen_index,
        screens,
        *tables,
    )
    return out.reshape(1, ROWS, 2, SLAB)


def solution(mesh):
    return jax.shard_map(
        functools.partial(body, mesh.shape["facet"], mesh.shape["col"]),
        mesh=mesh,
        in_specs=(P("facet", "col", None, None), P("col", None), P("col"), P("col", "facet"), P()),
        out_specs=P("facet", "col", None, None),
        check_vma=False,
    )
```

```python
import functools
import math

import jax
import jax.numpy as jnp
import numpy as np
from jax import lax
from jax.experimental import pallas as pl
from jax.experimental.pallas import tpu as pltpu
from jax.sharding import PartitionSpec as P

XC = 64
XS = 256
SLAB = 128
NPAD = 8192
STEP = 7
ROWS = 8
SPAN = 176
MESH = pl.DeviceIdType.MESH
F32 = jnp.float32
BF16 = jnp.bfloat16


def fourier_tables(facets):
    a = np.arange(XS)[:, None]
    q = np.arange(XS)[None, :]
    angle = 2.0 * np.pi * ((a * q) % XS) / XS
    keep = (q < STEP * (facets - 1) + XC).astype(np.float64)
    re = np.cos(angle) / math.sqrt(XS) * keep
    im = np.sin(angle) / math.sqrt(XS) * keep
    row_in = np.block([[re.T, im.T], [-im.T, re.T]])
    col_in = np.concatenate([re, im], axis=0) / math.sqrt(facets)
    col_out = np.concatenate([re.T[:SPAN], im.T[:SPAN]], axis=0)
    row_out = np.block([[re, -im], [im, re]])
    return tuple(jnp.asarray(t, dtype=BF16) for t in (row_in, col_in, col_out, row_out))


def unit_circle(n):
    n = n & (NPAD - 1)
    quarter = (n + NPAD // 8) >> 11
    t = (n - (quarter << 11)).astype(F32) * (2.0 * math.pi / NPAD)
    t2 = t * t
    c = 1.0 + t2 * (-1.0 / 2 + t2 * (1.0 / 24 + t2 * (-1.0 / 720 + t2 * (1.0 / 40320))))
    s = t * (1.0 + t2 * (-1.0 / 6 + t2 * (1.0 / 120 + t2 * (-1.0 / 5040 + t2 * (1.0 / 362880)))))
    odd = (quarter & 1) == 1
    cos = jnp.where(odd, s, c)
    sin = jnp.where(odd, c, s)
    cos = jnp.where(((quarter + 1) & 2) == 2, -cos, cos)
    sin = jnp.where((quarter & 2) == 2, -sin, sin)
    return cos, sin


def iota(shape, dim):
    return lax.broadcasted_iota(jnp.int32, shape, dim)


def join_parts(t):
    rows = t.shape[0]
    even = (iota(t.shape, 0) & 1) == 0
    low = iota(t.shape, 1) < XC
    other = jnp.where(even, pltpu.roll(t, rows - 1, 0), pltpu.roll(t, 1, 0))
    other = pltpu.roll(other, XC, 1)
    return jnp.where(even == low, t - other, t + other)


def dot(a, b):
    return jnp.dot(a, b, preferred_element_type=F32)


def peers_of_col(me, count):
    ny = count // 4
    steps = [(dy, low) for dy in range(ny) for low in range(4) if dy or low]
    steps.sort(key=lambda k: -(min(k[0], ny - k[0]) + (k[1] >> 1)))
    y, rest = me >> 2, me & 3
    return [lax.rem(y + dy, ny) * 4 + (rest ^ low) for dy, low in steps]


def peers_of_facet(me, count):
    nz = count // 2
    steps = [(dx, dz) for dx in range(2) for dz in range(nz) if dx or dz]
    steps.sort(key=lambda k: -(min(k[1], nz - k[1]) + 2 * k[0]))
    x, z = me // nz, lax.rem(me, nz)
    return [(x ^ dx) * nz + lax.rem(z + dz, nz) for dx, dz in steps]


def kernel(
    nf,
    nc,
    x_hbm,
    sub_hbm,
    col_hbm,
    idx_hbm,
    screens_hbm,
    row_in_hbm,
    col_in_hbm,
    col_out_hbm,
    row_out_hbm,
    out_ref,
    sub_s,
    col_s,
    idx_s,
    screens,
    row_in,
    col_in,
    col_out,
    row_out,
    slab,
    phase,
    phase_t,
    across,
    across_t,
    c_out,
    c_in,
    z,
    half,
    w,
    r_out,
    r_in,
    t_out,
    t_in,
    local_sem,
    slab_send,
    slab_recv,
    c_send,
    c_recv,
    r_send,
    r_recv,
    t_send,
    t_recv,
):
    me_f = lax.axis_index("facet")
    me_c = lax.axis_index("col")
    col_peers = peers_of_col(me_c, nc)
    facet_peers = peers_of_facet(me_f, nf)
    height = ROWS * nc
    block = 2 * ROWS

    def slab_rows(j):
        return pl.ds(pl.multiple_of(j * block, block), block)

    def sub_rows(s):
        return pl.ds(pl.multiple_of(s * XC, XC), XC)

    local = [
        pltpu.make_async_copy(src, dst, local_sem.at[i])
        for i, (src, dst) in enumerate(
            [
                (x_hbm, slab.at[slab_rows(me_c)]),
                (sub_hbm, sub_s),
                (col_hbm, col_s),
                (idx_hbm, idx_s),
                (screens_hbm, screens),
                (row_in_hbm, row_in),
                (col_in_hbm, col_in),
                (col_out_hbm, col_out),
                (row_out_hbm, row_out),
            ]
        )
    ]
    for copy in local:
        copy.start()

    barrier = pltpu.get_barrier_semaphore()

    for peer in col_peers:
        pl.semaphore_signal(barrier, 1, device_id={"col": peer}, device_id_type=MESH)
    for peer in facet_peers:
        pl.semaphore_signal(barrier, 1, device_id={"facet": peer}, device_id_type=MESH)

    local[0].wait()
    pl.semaphore_wait(barrier, nc - 1 + nf - 1)

    def remote(src, dst, send, recv, axis, peer):
        return pltpu.make_async_remote_copy(
            src_ref=src,
            dst_ref=dst,
            send_sem=send,
            recv_sem=recv,
            device_id={axis: peer},
            device_id_type=MESH,
        )

    mine = slab.at[slab_rows(me_c)]
    for peer in col_peers:
        remote(mine, mine, slab_send, slab_recv, "col", peer).start()

    for copy in local[1:4]:
        copy.wait()
    offset = col_s[0, 0]
    lane = iota((SLAB, 2 * XC), 1)
    cos, sin = unit_circle(iota((SLAB, 2 * XC), 0) * (offset + (lane & (XC - 1))))
    across[...] = (jnp.where(lane < XC, cos, -sin) * (1.0 / math.sqrt(SLAB))).astype(BF16)
    part = iota((2 * XC, SLAB), 0)
    cos, sin = unit_circle(iota((2 * XC, SLAB), 1) * (offset + (part & (XC - 1))))
    across_t[...] = (jnp.where(part < XC, cos, -sin) * (1.0 / math.sqrt(SLAB))).astype(BF16)

    lane_row = (8, 2 * height)
    place = iota(lane_row, 1)
    row_id = me_f * height + (place >> 1)
    turn = (place & 1) * (NPAD // 4)
    within = iota((XC, 2 * height), 0)
    place_u = iota((XC, 2 * height), 1)
    cos_u, sin_u = unit_circle(within * (me_f * height + (place_u >> 1)))
    cos_u = cos_u.reshape(XC // 8, 8, 2 * height)
    sin_u = sin_u.reshape(XC // 8, 8, 2 * height)

    def fill_phase(s, carry):
        cos_s, sin_s = unit_circle(sub_s[0, s] * row_id - turn)
        scale = 1.0 / math.sqrt(height)
        values = (cos_s * scale)[None] * cos_u - (sin_s * scale)[None] * sin_u
        phase[sub_rows(s), :] = values.reshape(XC, 2 * height).astype(BF16)
        return carry

    lax.fori_loop(0, nf, fill_phase, 0)

    tall = (2 * height, 2 * XC)
    row_t = me_f * height + (iota(tall, 0) >> 1)
    turn_t = (iota(tall, 0) & 1) * (NPAD // 4)
    lane_t = iota(tall, 1)

    def fill_phase_t(t, carry):
        freq = jnp.where(lane_t < XC, sub_s[0, 2 * t], sub_s[0, 2 * t + 1]) + (lane_t & (XC - 1))
        cos_t, _ = unit_circle(freq * row_t - turn_t)
        columns = pl.ds(pl.multiple_of(t * 2 * XC, 2 * XC), 2 * XC)
        phase_t[:, columns] = (cos_t * (1.0 / math.sqrt(height))).astype(BF16)
        return carry

    lax.fori_loop(0, nf // 2, fill_phase_t, 0)
    z[...] = jnp.zeros_like(z)
    half[...] = jnp.zeros_like(half)
    for copy in local[4:]:
        copy.wait()

    others = slab.at[pl.ds(0, (nc - 1) * block)]
    arrival = remote(others, others, slab_send, slab_recv, "col", me_c)
    arrival.wait_send()
    arrival.wait_recv()

    spread = join_parts(dot(slab[...], across[...])).astype(BF16)
    c_out[...] = dot(phase[...], spread).astype(BF16)

    for peer in facet_peers:
        remote(
            c_out.at[sub_rows(peer)], c_in.at[sub_rows(me_f)], c_send, c_recv.at[me_f], "facet", peer
        ).start()
    c_in[sub_rows(me_f), :] = c_out[sub_rows(me_f), :]

    lane_c = iota((XC, 2 * XC), 1)
    for f in range(nf):
        start = STEP * f
        rows = pl.ds(start, XC)

        @pl.when(f != me_f)
        def _():
            slot = c_in.at[pl.ds(f * XC, XC)]
            remote(slot, slot, c_send, c_recv.at[f], "facet", me_f).wait_recv()

        got = c_in[pl.ds(f * XC, XC), :].astype(F32)
        re = pltpu.roll(got, start, 1) if start else got
        im = pltpu.roll(got, (start + XC) % (2 * XC), 1)
        first = (lane_c >= start) & (lane_c < start + XC)
        z[rows, 0:128] += jnp.where(first, re, 0.0)
        z[rows, 256:384] += jnp.where(first, im, 0.0)
        if start + XC > 128:
            second = lane_c < start + XC - 128
            z[rows, 128:256] += jnp.where(second, re, 0.0)
            z[rows, 384:512] += jnp.where(second, im, 0.0)

    half[0:SPAN, :] = dot(z[...].astype(BF16), row_in[...]).astype(BF16)
    grid = dot(col_in[...], half[...])
    sub_re = grid[0:XS, 0:XS] - grid[XS:, XS:]
    sub_im = grid[0:XS, XS:] + grid[XS:, 0:XS]
    g = idx_s[0, 0]
    gain_re = screens[g, 0]
    gain_im = screens[g, 1]
    screened = jnp.concatenate(
        [
            (sub_re * gain_re - sub_im * gain_im).astype(BF16),
            (sub_re * gain_im + sub_im * gain_re).astype(BF16),
        ],
        axis=1,
    )
    inner = dot(col_out[...], screened)
    inner = jnp.concatenate(
        [
            (inner[0:SPAN, 0:XS] + inner[SPAN:, XS:]).astype(BF16),
            (inner[0:SPAN, XS:] - inner[SPAN:, 0:XS]).astype(BF16),
        ],
        axis=1,
    )
    w[...] = dot(inner, row_out[...])

    for f in range(nf):
        start = STEP * f
        rows = pl.ds(start, XC)
        re = w[rows, 0:128]
        im = w[rows, 256:384]
        if start + XC > 128:
            re = jnp.where(lane_c >= start, re, w[rows, 128:256])
            im = jnp.where(lane_c >= start, im, w[rows, 384:512])
        re = pltpu.roll(re, 128 - start, 1) if start else re
        im = pltpu.roll(im, (XC + 128 - start) % 128, 1)
        r_out[pl.ds(f * XC, XC), :] = jnp.where(lane_c < XC, re, im).astype(BF16)

    for peer in facet_peers:
        remote(
            r_out.at[sub_rows(peer)], r_in.at[sub_rows(me_f)], r_send, r_recv, "facet", peer
        ).start()
    r_in[sub_rows(me_f), :] = r_out[sub_rows(me_f), :]

    others = r_in.at[pl.ds(0, (nf - 1) * XC)]
    remote(others, others, r_send, r_recv, "facet", me_f).wait_recv()

    rows = join_parts(dot(phase_t[...], r_in[...])).astype(BF16)
    t_out[...] = dot(rows, across_t[...]).astype(BF16)

    for peer in col_peers:
        remote(
            t_out.at[slab_rows(peer)], t_in.at[slab_rows(me_c)], t_send, t_recv, "col", peer
        ).start()
    t_in[slab_rows(me_c), :] = t_out[slab_rows(me_c), :]

    others = c_in.at[pl.ds(0, (nf - 1) * XC)]
    remote(others, others, c_send, r_recv, "facet", me_f).wait_send()
    remote(others, others, r_send, r_recv, "facet", me_f).wait_send()
    others = t_in.at[pl.ds(0, (nc - 1) * block)]
    arrival = remote(others, others, t_send, t_recv, "col", me_c)
    arrival.wait_send()
    arrival.wait_recv()

    total = jnp.sum(t_in[...].astype(F32).reshape(nc, block, SLAB), axis=0)
    out_ref[...] = total * (1.0 / math.sqrt(nc * nf))


def body(nf, nc, facets, sub_offsets, col_offsets, screen_index, screens):
    block = 2 * ROWS
    height = ROWS * nc
    tables = fourier_tables(nf)
    hbm = pl.BlockSpec(memory_space=pltpu.HBM)
    vmem = pltpu.VMEM
    dma = pltpu.SemaphoreType.DMA
    out = pl.pallas_call(
        functools.partial(kernel, nf, nc),
        name="swiftly",
        out_shape=jax.ShapeDtypeStruct((block, SLAB), F32),
        in_specs=[hbm] * 9,
        out_specs=pl.BlockSpec(memory_space=pltpu.VMEM),
        scratch_shapes=[
            pltpu.SMEM((1, nf), jnp.int32),
            pltpu.SMEM((1, 1), jnp.int32),
            pltpu.SMEM((1, 1), jnp.int32),
            vmem(screens.shape, F32),
            *[vmem(t.shape, BF16) for t in tables],
            vmem((2 * height, SLAB), BF16),
            vmem((nf * XC, 2 * height), BF16),
            vmem((2 * height, nf * XC), BF16),
            vmem((SLAB, 2 * XC), BF16),
            vmem((2 * XC, SLAB), BF16),
            vmem((nf * XC, 2 * XC), BF16),
            vmem((nf * XC, 2 * XC), BF16),
            vmem((SPAN, 2 * XS), F32),
            vmem((XS, 2 * XS), BF16),
            vmem((SPAN, 2 * XS), F32),
            vmem((nf * XC, 2 * XC), BF16),
            vmem((nf * XC, 2 * XC), BF16),
            vmem((2 * height, SLAB), BF16),
            vmem((2 * height, SLAB), BF16),
            dma((9,)),
            dma,
            dma,
            dma,
            dma((nf,)),
            dma,
            dma,
            dma,
            dma,
        ],
        compiler_params=pltpu.CompilerParams(collective_id=0, has_side_effects=True),
    )(
        facets.reshape(block, SLAB),
        sub_offsets,
        col_offsets.reshape(1, 1),
        screen_index,
        screens,
        *tables,
    )
    return out.reshape(1, ROWS, 2, SLAB)


def solution(mesh):
    return jax.shard_map(
        functools.partial(body, mesh.shape["facet"], mesh.shape["col"]),
        mesh=mesh,
        in_specs=(P("facet", "col", None, None), P("col", None), P("col"), P("col", "facet"), P()),
        out_specs=P("facet", "col", None, None),
        check_vma=False,
    )
```

```python
import functools
import math

import jax
import jax.numpy as jnp
import numpy as np
from jax import lax
from jax.experimental import pallas as pl
from jax.experimental.pallas import tpu as pltpu
from jax.sharding import PartitionSpec as P

XC = 64
XS = 256
SLAB = 128
NPAD = 8192
STEP = 7
ROWS = 8
SPAN = 176
BLOCKS = 3
MESH = pl.DeviceIdType.MESH
F32 = jnp.float32
BF16 = jnp.bfloat16


def fourier_tables(facets):
    a = np.arange(XS)[:, None]
    q = np.arange(XS)[None, :]
    angle = 2.0 * np.pi * ((a * q) % XS) / XS
    keep = (q < STEP * (facets - 1) + XC).astype(np.float64)
    re = np.cos(angle) / math.sqrt(XS) * keep
    im = np.sin(angle) / math.sqrt(XS) * keep
    across = np.block([[re.T, im.T], [-im.T, re.T]])
    order = np.arange(BLOCKS * 2 * XC)
    order = order // (2 * XC) * XC + order % XC + order // XC % 2 * XS
    row_in = across[order]
    col_in = np.concatenate([re, im], axis=0) / math.sqrt(facets)
    col_out = np.concatenate([re.T[:SPAN], im.T[:SPAN]], axis=0)
    row_out = np.block([[re, -im], [im, re]])[:, order]
    return tuple(jnp.asarray(t, dtype=BF16) for t in (row_in, col_in, col_out, row_out))


def unit_circle(n):
    n = n & (NPAD - 1)
    quarter = (n + NPAD // 8) >> 11
    t = (n - (quarter << 11)).astype(F32) * (2.0 * math.pi / NPAD)
    t2 = t * t
    c = 1.0 + t2 * (-1.0 / 2 + t2 * (1.0 / 24 + t2 * (-1.0 / 720 + t2 * (1.0 / 40320))))
    s = t * (1.0 + t2 * (-1.0 / 6 + t2 * (1.0 / 120 + t2 * (-1.0 / 5040 + t2 * (1.0 / 362880)))))
    odd = (quarter & 1) == 1
    cos = jnp.where(odd, s, c)
    sin = jnp.where(odd, c, s)
    cos = jnp.where(((quarter + 1) & 2) == 2, -cos, cos)
    sin = jnp.where((quarter & 2) == 2, -sin, sin)
    return cos, sin


def iota(shape, dim):
    return lax.broadcasted_iota(jnp.int32, shape, dim)


def join_parts(t):
    rows = t.shape[0]
    even = (iota(t.shape, 0) & 1) == 0
    low = iota(t.shape, 1) < XC
    other = jnp.where(even, pltpu.roll(t, rows - 1, 0), pltpu.roll(t, 1, 0))
    other = pltpu.roll(other, XC, 1)
    return jnp.where(even == low, t - other, t + other)


def dot(a, b):
    return jnp.dot(a, b, preferred_element_type=F32)


def peers_of_col(me, count):
    ny = count // 4
    steps = [(dy, low) for dy in range(ny) for low in range(4) if dy or low]
    steps.sort(key=lambda k: -(min(k[0], ny - k[0]) + (k[1] >> 1)))
    y, rest = me >> 2, me & 3
    return [lax.rem(y + dy, ny) * 4 + (rest ^ low) for dy, low in steps]


def peers_of_facet(me, count):
    nz = count // 2
    steps = [(dx, dz) for dx in range(2) for dz in range(nz) if dx or dz]
    steps.sort(key=lambda k: (-k[0], -min(k[1], nz - k[1])))
    x, z = me // nz, lax.rem(me, nz)
    return [(x ^ dx) * nz + lax.rem(z + dz, nz) for dx, dz in steps]


def kernel(
    nf,
    nc,
    x_hbm,
    sub_hbm,
    col_s,
    idx_s,
    screens_hbm,
    row_in_hbm,
    col_in_hbm,
    col_out_hbm,
    row_out_hbm,
    out_ref,
    sub_s,
    screens,
    row_in,
    col_in,
    col_out,
    row_out,
    slab,
    phase,
    phase_t,
    across,
    offs,
    back,
    c_out,
    c_in,
    z,
    half,
    w,
    r_out,
    r_in,
    t_out,
    t_in,
    local_sem,
    slab_send,
    slab_recv,
    offs_send,
    offs_recv,
    c_send,
    c_recv,
    r_send,
    r_recv,
    t_send,
    t_recv,
):
    me_f = lax.axis_index("facet")
    me_c = lax.axis_index("col")
    col_peers = peers_of_col(me_c, nc)
    facet_peers = peers_of_facet(me_f, nf)
    height = ROWS * nc
    block = 2 * ROWS

    def slab_rows(j):
        return pl.ds(pl.multiple_of(j * block, block), block)

    def sub_rows(s):
        return pl.ds(pl.multiple_of(s * XC, XC), XC)

    local = [
        pltpu.make_async_copy(src, dst, local_sem.at[i])
        for i, (src, dst) in enumerate(
            [
                (x_hbm, slab.at[slab_rows(me_c)]),
                (sub_hbm, sub_s),
                (screens_hbm, screens),
                (row_in_hbm, row_in),
                (col_in_hbm, col_in),
                (col_out_hbm, col_out),
                (row_out_hbm, row_out),
            ]
        )
    ]
    for copy in local:
        copy.start()

    offset = col_s[0]
    shift = STEP * me_f
    offs[me_c] = jnp.full((1, SLAB), offset, jnp.int32)

    barrier = pltpu.get_barrier_semaphore()

    for peer in col_peers:
        pl.semaphore_signal(barrier, 1, device_id={"col": peer}, device_id_type=MESH)
    for peer in facet_peers:
        pl.semaphore_signal(barrier, 1, device_id={"facet": peer}, device_id_type=MESH)

    local[0].wait()
    pl.semaphore_wait(barrier, nc - 1 + nf - 1)

    def remote(src, dst, send, recv, axis, peer):
        return pltpu.make_async_remote_copy(
            src_ref=src,
            dst_ref=dst,
            send_sem=send,
            recv_sem=recv,
            device_id={axis: peer},
            device_id_type=MESH,
        )

    mine = slab.at[slab_rows(me_c)]
    for peer in col_peers:
        remote(mine, mine, slab_send, slab_recv, "col", peer).start()

    lane = iota((SLAB, 2 * XC), 1)
    cos, sin = unit_circle(iota((SLAB, 2 * XC), 0) * (offset + ((lane - shift) & (XC - 1))))
    across[...] = (jnp.where(lane < XC, cos, -sin) * (1.0 / math.sqrt(SLAB))).astype(BF16)

    local[1].wait()
    lane_row = (8, 2 * height)
    place = iota(lane_row, 1)
    row_id = me_f * height + (place >> 1)
    turn = (place & 1) * (NPAD // 4)
    within = iota((XC, 2 * height), 0)
    place_u = iota((XC, 2 * height), 1)
    cos_u, sin_u = unit_circle(within * (me_f * height + (place_u >> 1)))
    cos_u = cos_u.reshape(XC // 8, 8, 2 * height)
    sin_u = sin_u.reshape(XC // 8, 8, 2 * height)

    def fill_phase(s, carry):
        cos_s, sin_s = unit_circle(sub_s[0, s] * row_id - turn)
        scale = 1.0 / math.sqrt(height)
        values = (cos_s * scale)[None] * cos_u - (sin_s * scale)[None] * sin_u
        phase[sub_rows(s), :] = values.reshape(XC, 2 * height).astype(BF16)
        return carry

    lax.fori_loop(0, nf, fill_phase, 0)

    tall = (2 * height, 2 * XC)
    place_t = iota(tall, 0)
    second_t = place_t >= height
    row_t = me_f * height + jnp.where(second_t, place_t - height, place_t)
    turn_t = jnp.where(second_t, NPAD // 4, 0)
    lane_t = iota(tall, 1)

    def fill_phase_t(t, carry):
        freq = jnp.where(lane_t < XC, sub_s[0, 2 * t], sub_s[0, 2 * t + 1]) + (lane_t & (XC - 1))
        cos_t, _ = unit_circle(freq * row_t - turn_t)
        columns = pl.ds(pl.multiple_of(t * 2 * XC, 2 * XC), 2 * XC)
        phase_t[:, columns] = (cos_t * (1.0 / math.sqrt(height))).astype(BF16)
        return carry

    lax.fori_loop(0, nf // 2, fill_phase_t, 0)
    z[...] = jnp.zeros_like(z)
    half[...] = jnp.zeros_like(half)
    for copy in local[2:]:
        copy.wait()

    others = slab.at[pl.ds(0, (nc - 1) * block)]
    arrival = remote(others, others, slab_send, slab_recv, "col", me_c)
    arrival.wait_send()
    arrival.wait_recv()

    spread = join_parts(dot(slab[...], across[...])).astype(BF16)
    half_rows = nf // 2 * XC
    far_half = (me_f // (nf // 2)) ^ 1
    for group in range(2):
        rows = pl.ds(pl.multiple_of((far_half ^ group) * half_rows, half_rows), half_rows)
        c_out[rows, :] = dot(phase[rows, :], spread).astype(BF16)
        for peer in facet_peers[nf // 2 * group : nf // 2 * (group + 1)]:
            remote(
                c_out.at[sub_rows(peer)],
                c_in.at[sub_rows(me_f)],
                c_send,
                c_recv.at[me_f],
                "facet",
                peer,
            ).start()
    c_in[sub_rows(me_f), :] = c_out[sub_rows(me_f), :]

    mine = offs.at[me_c]
    for peer in col_peers:
        remote(mine, mine, offs_send, offs_recv, "col", peer).start()

    lane_v = iota((XC, 2 * XC), 1) & (XC - 1)
    for f in range(nf):
        start = STEP * f
        first, inside = divmod(start, XC)
        rows = pl.ds(start, XC)

        @pl.when(f != me_f)
        def _():
            slot = c_in.at[pl.ds(f * XC, XC)]
            remote(slot, slot, c_send, c_recv.at[f], "facet", me_f).wait_recv()

        got = c_in[pl.ds(f * XC, XC), :].astype(F32)
        if inside:
            z[first, rows, :] += jnp.where(lane_v >= inside, got, 0.0)
            z[first + 1, rows, :] += jnp.where(lane_v >= inside, 0.0, got)
        else:
            z[first, rows, :] += got

    placed = jnp.concatenate([z[b].astype(BF16) for b in range(BLOCKS)], axis=1)
    half[0:SPAN, :] = dot(placed, row_in[...]).astype(BF16)
    grid = dot(col_in[...], half[...])
    sub_re = grid[0:XS, 0:XS] - grid[XS:, XS:]
    sub_im = grid[0:XS, XS:] + grid[XS:, 0:XS]
    g = idx_s[0, 0]
    gain_re = screens[g, 0]
    gain_im = screens[g, 1]
    screened = jnp.concatenate(
        [
            (sub_re * gain_re - sub_im * gain_im).astype(BF16),
            (sub_re * gain_im + sub_im * gain_re).astype(BF16),
        ],
        axis=1,
    )
    inner = dot(col_out[...], screened)
    inner = jnp.concatenate(
        [
            (inner[0:SPAN, 0:XS] + inner[SPAN:, XS:]).astype(BF16),
            (inner[0:SPAN, XS:] - inner[SPAN:, 0:XS]).astype(BF16),
        ],
        axis=1,
    )
    windows = dot(inner, row_out[...])
    for b in range(BLOCKS):
        w[b] = windows[:, b * 2 * XC : (b + 1) * 2 * XC]

    for f in range(nf):
        start = STEP * f
        first, inside = divmod(start, XC)
        rows = pl.ds(start, XC)
        cut = w[first, rows, :]
        if inside:
            cut = jnp.where(lane_v >= inside, cut, w[first + 1, rows, :])
        r_out[pl.ds(f * XC, XC), :] = cut.astype(BF16)

    for peer in facet_peers:
        remote(
            r_out.at[sub_rows(peer)], r_in.at[sub_rows(me_f)], r_send, r_recv, "facet", peer
        ).start()
    r_in[sub_rows(me_f), :] = r_out[sub_rows(me_f), :]

    others = offs.at[pl.ds(0, nc - 1)]
    arrival = remote(others, others, offs_send, offs_recv, "col", me_c)
    arrival.wait_send()
    arrival.wait_recv()
    at_x = iota((XC, SLAB), 1)
    at_v = (iota((XC, SLAB), 0) - shift) & (XC - 1)

    def fill_across(j, carry):
        cos_j, sin_j = unit_circle(at_x * (offs[j] + at_v))
        cos_j = cos_j * (1.0 / math.sqrt(SLAB))
        sin_j = sin_j * (1.0 / math.sqrt(SLAB))
        back[j, 0:XC, 0:SLAB] = cos_j.astype(BF16)
        back[j, 0:XC, SLAB:] = sin_j.astype(BF16)
        back[j, XC:, 0:SLAB] = (-sin_j).astype(BF16)
        back[j, XC:, SLAB:] = cos_j.astype(BF16)
        return carry

    lax.fori_loop(0, nc, fill_across, 0)

    others = r_in.at[pl.ds(0, (nf - 1) * XC)]
    remote(others, others, r_send, r_recv, "facet", me_f).wait_recv()

    terms = dot(phase_t[...], r_in[...])
    turned = pltpu.roll(terms[height:], XC, 1)
    rows = terms[0:height] + jnp.where(iota((height, 2 * XC), 1) < XC, -turned, turned)
    t_out[...] = rows.reshape(nc, ROWS, 2 * XC).astype(BF16)
    for peer in col_peers:
        remote(t_out.at[peer], t_in.at[me_c], t_send, t_recv.at[me_c], "col", peer).start()

    others = c_in.at[pl.ds(0, (nf - 1) * XC)]
    remote(others, others, c_send, r_recv, "facet", me_f).wait_send()
    remote(others, others, r_send, r_recv, "facet", me_f).wait_send()

    total = dot(t_out[me_c], back[me_c])
    near_first = col_peers[::-1]
    cut = 3 * nc // 4
    for group in (near_first[:cut], near_first[cut:]):
        for peer in group:
            slot = t_in.at[peer]
            remote(slot, slot, t_send, t_recv.at[peer], "col", me_c).wait_recv()
        for peer in group:
            total += dot(t_in[peer], back[peer])
    total = total * (1.0 / math.sqrt(nc * nf))
    out_ref[pl.ds(0, ROWS, stride=2), :] = total[:, 0:SLAB]
    out_ref[pl.ds(1, ROWS, stride=2), :] = total[:, SLAB:]

    others = t_in.at[pl.ds(0, nc - 1)]
    remote(others, others, t_send, r_recv, "col", me_c).wait_send()


def body(nf, nc, facets, sub_offsets, col_offsets, screen_index, screens):
    block = 2 * ROWS
    height = ROWS * nc
    tables = fourier_tables(nf)
    hbm = pl.BlockSpec(memory_space=pltpu.HBM)
    smem = pl.BlockSpec(memory_space=pltpu.SMEM)
    vmem = pltpu.VMEM
    dma = pltpu.SemaphoreType.DMA
    out = pl.pallas_call(
        functools.partial(kernel, nf, nc),
        name="swiftly",
        out_shape=jax.ShapeDtypeStruct((block, SLAB), F32),
        in_specs=[hbm, hbm, smem, smem] + [hbm] * 5,
        out_specs=pl.BlockSpec(memory_space=pltpu.VMEM),
        scratch_shapes=[
            pltpu.SMEM((1, nf), jnp.int32),
            vmem(screens.shape, F32),
            *[vmem(t.shape, BF16) for t in tables],
            vmem((2 * height, SLAB), BF16),
            vmem((nf * XC, 2 * height), BF16),
            vmem((2 * height, nf * XC), BF16),
            vmem((SLAB, 2 * XC), BF16),
            vmem((nc, 1, SLAB), jnp.int32),
            vmem((nc, 2 * XC, 2 * SLAB), BF16),
            vmem((nf * XC, 2 * XC), BF16),
            vmem((nf * XC, 2 * XC), BF16),
            vmem((BLOCKS, SPAN, 2 * XC), F32),
            vmem((XS, 2 * XS), BF16),
            vmem((BLOCKS, SPAN, 2 * XC), F32),
            vmem((nf * XC, 2 * XC), BF16),
            vmem((nf * XC, 2 * XC), BF16),
            vmem((nc, ROWS, 2 * XC), BF16),
            vmem((nc, ROWS, 2 * XC), BF16),
            dma((7,)),
            dma,
            dma,
            dma,
            dma,
            dma,
            dma((nf,)),
            dma,
            dma,
            dma,
            dma((nc,)),
        ],
        compiler_params=pltpu.CompilerParams(collective_id=0, has_side_effects=True),
    )(
        facets.reshape(block, SLAB),
        sub_offsets,
        col_offsets,
        screen_index,
        screens,
        *tables,
    )
    return out.reshape(1, ROWS, 2, SLAB)


def solution(mesh):
    return jax.shard_map(
        functools.partial(body, mesh.shape["facet"], mesh.shape["col"]),
        mesh=mesh,
        in_specs=(P("facet", "col", None, None), P("col", None), P("col"), P("col", "facet"), P()),
        out_specs=P("facet", "col", None, None),
        check_vma=False,
    )
```

```python
import functools
import math

import jax
import jax.numpy as jnp
import numpy as np
from jax import lax
from jax.experimental import pallas as pl
from jax.experimental.pallas import tpu as pltpu
from jax.sharding import PartitionSpec as P

XC = 64
XS = 256
SLAB = 128
NPAD = 8192
STEP = 7
ROWS = 8
SPAN = 176
BLOCKS = 3
MESH = pl.DeviceIdType.MESH
F32 = jnp.float32
BF16 = jnp.bfloat16


def fourier_tables(facets):
    a = np.arange(XS)[:, None]
    q = np.arange(XS)[None, :]
    angle = 2.0 * np.pi * ((a * q) % XS) / XS
    keep = (q < STEP * (facets - 1) + XC).astype(np.float64)
    re = np.cos(angle) / math.sqrt(XS) * keep
    im = np.sin(angle) / math.sqrt(XS) * keep
    across = np.block([[re.T, im.T], [-im.T, re.T]])
    order = np.arange(BLOCKS * 2 * XC)
    order = order // (2 * XC) * XC + order % XC + order // XC % 2 * XS
    row_in = across[order]
    col_in = np.concatenate([re, im], axis=0) / math.sqrt(facets)
    col_out = np.concatenate([re.T[:SPAN], im.T[:SPAN]], axis=0)
    row_out = np.block([[re, -im], [im, re]])[:, order]
    return tuple(jnp.asarray(t, dtype=BF16) for t in (row_in, col_in, col_out, row_out))


def unit_circle(n):
    n = n & (NPAD - 1)
    quarter = (n + NPAD // 8) >> 11
    t = (n - (quarter << 11)).astype(F32) * (2.0 * math.pi / NPAD)
    t2 = t * t
    c = 1.0 + t2 * (-1.0 / 2 + t2 * (1.0 / 24 + t2 * (-1.0 / 720 + t2 * (1.0 / 40320))))
    s = t * (1.0 + t2 * (-1.0 / 6 + t2 * (1.0 / 120 + t2 * (-1.0 / 5040 + t2 * (1.0 / 362880)))))
    odd = (quarter & 1) == 1
    cos = jnp.where(odd, s, c)
    sin = jnp.where(odd, c, s)
    cos = jnp.where(((quarter + 1) & 2) == 2, -cos, cos)
    sin = jnp.where((quarter & 2) == 2, -sin, sin)
    return cos, sin


def iota(shape, dim):
    return lax.broadcasted_iota(jnp.int32, shape, dim)


def join_parts(t):
    rows = t.shape[0]
    even = (iota(t.shape, 0) & 1) == 0
    low = iota(t.shape, 1) < XC
    other = jnp.where(even, pltpu.roll(t, rows - 1, 0), pltpu.roll(t, 1, 0))
    other = pltpu.roll(other, XC, 1)
    return jnp.where(even == low, t - other, t + other)


def dot(a, b):
    return jnp.dot(a, b, preferred_element_type=F32)


def peers_of_col(me, count):
    ny = count // 4
    steps = [(dy, low) for dy in range(ny) for low in range(4) if dy or low]
    steps.sort(key=lambda k: -(min(k[0], ny - k[0]) + (k[1] >> 1)))
    y, rest = me >> 2, me & 3
    return [lax.rem(y + dy, ny) * 4 + (rest ^ low) for dy, low in steps]


def peers_of_facet(me, count):
    nz = count // 2
    steps = [(dx, dz) for dx in range(2) for dz in range(nz) if dx or dz]
    steps.sort(key=lambda k: (-k[0], -min(k[1], nz - k[1])))
    x, z = me // nz, lax.rem(me, nz)
    by_x = [(x ^ dx) * nz + lax.rem(z + dz, nz) for dx, dz in steps]
    steps.sort(key=lambda k: -(min(k[1], nz - k[1]) + 2 * k[0]))
    return by_x, [(x ^ dx) * nz + lax.rem(z + dz, nz) for dx, dz in steps]


def kernel(
    nf,
    nc,
    x_hbm,
    sub_hbm,
    col_s,
    idx_s,
    screens_hbm,
    row_in_hbm,
    col_in_hbm,
    col_out_hbm,
    row_out_hbm,
    out_ref,
    sub_s,
    screens,
    row_in,
    col_in,
    col_out,
    row_out,
    slab,
    phase,
    phase_t,
    across,
    offs,
    back,
    c_out,
    c_in,
    z,
    half,
    w,
    r_out,
    r_in,
    t_out,
    t_in,
    local_sem,
    slab_send,
    slab_recv,
    offs_send,
    offs_recv,
    c_send,
    c_recv,
    r_send,
    r_recv,
    t_send,
    t_recv,
):
    me_f = lax.axis_index("facet")
    me_c = lax.axis_index("col")
    col_peers = peers_of_col(me_c, nc)
    facet_peers, facet_far = peers_of_facet(me_f, nf)
    height = ROWS * nc
    block = 2 * ROWS

    def slab_rows(j):
        return pl.ds(pl.multiple_of(j * block, block), block)

    def sub_rows(s):
        return pl.ds(pl.multiple_of(s * XC, XC), XC)

    local = [
        pltpu.make_async_copy(src, dst, local_sem.at[i])
        for i, (src, dst) in enumerate(
            [
                (x_hbm, slab.at[slab_rows(me_c)]),
                (sub_hbm, sub_s),
                (screens_hbm, screens),
                (row_in_hbm, row_in),
                (col_in_hbm, col_in),
                (col_out_hbm, col_out),
                (row_out_hbm, row_out),
            ]
        )
    ]
    for copy in local:
        copy.start()

    offset = col_s[0]
    shift = STEP * me_f
    offs[me_c] = jnp.full((1, SLAB), offset, jnp.int32)

    barrier = pltpu.get_barrier_semaphore()

    for peer in col_peers:
        pl.semaphore_signal(barrier, 1, device_id={"col": peer}, device_id_type=MESH)
    for peer in facet_peers:
        pl.semaphore_signal(barrier, 1, device_id={"facet": peer}, device_id_type=MESH)

    local[0].wait()
    pl.semaphore_wait(barrier, nc - 1 + nf - 1)

    def remote(src, dst, send, recv, axis, peer):
        return pltpu.make_async_remote_copy(
            src_ref=src,
            dst_ref=dst,
            send_sem=send,
            recv_sem=recv,
            device_id={axis: peer},
            device_id_type=MESH,
        )

    mine = slab.at[slab_rows(me_c)]
    for peer in col_peers:
        remote(mine, mine, slab_send, slab_recv, "col", peer).start()

    lane = iota((SLAB, 2 * XC), 1)
    cos, sin = unit_circle(iota((SLAB, 2 * XC), 0) * (offset + ((lane - shift) & (XC - 1))))
    across[...] = (jnp.where(lane < XC, cos, -sin) * (1.0 / math.sqrt(SLAB))).astype(BF16)

    local[1].wait()
    lane_row = (8, 2 * height)
    place = iota(lane_row, 1)
    row_id = me_f * height + (place >> 1)
    turn = (place & 1) * (NPAD // 4)
    within = iota((XC, 2 * height), 0)
    place_u = iota((XC, 2 * height), 1)
    cos_u, sin_u = unit_circle(within * (me_f * height + (place_u >> 1)))
    cos_u = cos_u.reshape(XC // 8, 8, 2 * height)
    sin_u = sin_u.reshape(XC // 8, 8, 2 * height)

    def fill_phase(s, carry):
        cos_s, sin_s = unit_circle(sub_s[0, s] * row_id - turn)
        scale = 1.0 / math.sqrt(height)
        values = (cos_s * scale)[None] * cos_u - (sin_s * scale)[None] * sin_u
        phase[sub_rows(s), :] = values.reshape(XC, 2 * height).astype(BF16)
        return carry

    lax.fori_loop(0, nf, fill_phase, 0)

    tall = (2 * height, 2 * XC)
    place_t = iota(tall, 0)
    second_t = place_t >= height
    row_t = me_f * height + jnp.where(second_t, place_t - height, place_t)
    turn_t = jnp.where(second_t, NPAD // 4, 0)
    lane_t = iota(tall, 1)

    def fill_phase_t(t, carry):
        freq = jnp.where(lane_t < XC, sub_s[0, 2 * t], sub_s[0, 2 * t + 1]) + (lane_t & (XC - 1))
        cos_t, _ = unit_circle(freq * row_t - turn_t)
        columns = pl.ds(pl.multiple_of(t * 2 * XC, 2 * XC), 2 * XC)
        phase_t[:, columns] = (cos_t * (1.0 / math.sqrt(height))).astype(BF16)
        return carry

    lax.fori_loop(0, nf // 2, fill_phase_t, 0)
    z[...] = jnp.zeros_like(z)
    half[...] = jnp.zeros_like(half)
    for copy in local[2:]:
        copy.wait()

    others = slab.at[pl.ds(0, (nc - 1) * block)]
    arrival = remote(others, others, slab_send, slab_recv, "col", me_c)
    arrival.wait_send()
    arrival.wait_recv()

    spread = join_parts(dot(slab[...], across[...])).astype(BF16)
    half_rows = nf // 2 * XC
    far_half = (me_f // (nf // 2)) ^ 1
    for group in range(2):
        rows = pl.ds(pl.multiple_of((far_half ^ group) * half_rows, half_rows), half_rows)
        c_out[rows, :] = dot(phase[rows, :], spread).astype(BF16)
        for peer in facet_peers[nf // 2 * group : nf // 2 * (group + 1)]:
            remote(
                c_out.at[sub_rows(peer)],
                c_in.at[sub_rows(me_f)],
                c_send,
                c_recv.at[me_f],
                "facet",
                peer,
            ).start()
    c_in[sub_rows(me_f), :] = c_out[sub_rows(me_f), :]

    mine = offs.at[me_c]
    for peer in col_peers:
        remote(mine, mine, offs_send, offs_recv, "col", peer).start()

    others = offs.at[pl.ds(0, nc - 1)]
    arrival = remote(others, others, offs_send, offs_recv, "col", me_c)
    arrival.wait_send()
    arrival.wait_recv()
    at_x = iota((XC, SLAB), 1)
    at_v = (iota((XC, SLAB), 0) - shift) & (XC - 1)

    def fill_across(j, carry):
        cos_j, sin_j = unit_circle(at_x * (offs[j] + at_v))
        cos_j = cos_j * (1.0 / math.sqrt(SLAB))
        sin_j = sin_j * (1.0 / math.sqrt(SLAB))
        back[j, 0:XC, 0:SLAB] = cos_j.astype(BF16)
        back[j, 0:XC, SLAB:] = sin_j.astype(BF16)
        back[j, XC:, 0:SLAB] = (-sin_j).astype(BF16)
        back[j, XC:, SLAB:] = cos_j.astype(BF16)
        return carry

    lax.fori_loop(0, nc, fill_across, 0)

    lane_v = iota((XC, 2 * XC), 1) & (XC - 1)
    for f in range(nf):
        start = STEP * f
        first, inside = divmod(start, XC)
        rows = pl.ds(start, XC)

        @pl.when(f != me_f)
        def _():
            slot = c_in.at[pl.ds(f * XC, XC)]
            remote(slot, slot, c_send, c_recv.at[f], "facet", me_f).wait_recv()

        got = c_in[pl.ds(f * XC, XC), :].astype(F32)
        if inside:
            z[first, rows, :] += jnp.where(lane_v >= inside, got, 0.0)
            z[first + 1, rows, :] += jnp.where(lane_v >= inside, 0.0, got)
        else:
            z[first, rows, :] += got

    placed = jnp.concatenate([z[b].astype(BF16) for b in range(BLOCKS)], axis=1)
    half[0:SPAN, :] = dot(placed, row_in[...]).astype(BF16)
    grid = dot(col_in[...], half[...])
    sub_re = grid[0:XS, 0:XS] - grid[XS:, XS:]
    sub_im = grid[0:XS, XS:] + grid[XS:, 0:XS]
    g = idx_s[0, 0]
    gain_re = screens[g, 0]
    gain_im = screens[g, 1]
    screened = jnp.concatenate(
        [
            (sub_re * gain_re - sub_im * gain_im).astype(BF16),
            (sub_re * gain_im + sub_im * gain_re).astype(BF16),
        ],
        axis=1,
    )
    inner = dot(col_out[...], screened)
    inner = jnp.concatenate(
        [
            (inner[0:SPAN, 0:XS] + inner[SPAN:, XS:]).astype(BF16),
            (inner[0:SPAN, XS:] - inner[SPAN:, 0:XS]).astype(BF16),
        ],
        axis=1,
    )
    windows = dot(inner, row_out[...])
    for b in range(BLOCKS):
        w[b] = windows[:, b * 2 * XC : (b + 1) * 2 * XC]

    for f in range(nf):
        start = STEP * f
        first, inside = divmod(start, XC)
        rows = pl.ds(start, XC)
        cut = w[first, rows, :]
        if inside:
            cut = jnp.where(lane_v >= inside, cut, w[first + 1, rows, :])
        r_out[pl.ds(f * XC, XC), :] = cut.astype(BF16)

    for peer in facet_far:
        remote(
            r_out.at[sub_rows(peer)], r_in.at[sub_rows(me_f)], r_send, r_recv, "facet", peer
        ).start()
    r_in[sub_rows(me_f), :] = r_out[sub_rows(me_f), :]

    others = r_in.at[pl.ds(0, (nf - 1) * XC)]
    remote(others, others, r_send, r_recv, "facet", me_f).wait_recv()

    terms = dot(phase_t[...], r_in[...])
    turned = pltpu.roll(terms[height:], XC, 1)
    rows = terms[0:height] + jnp.where(iota((height, 2 * XC), 1) < XC, -turned, turned)
    t_out[...] = rows.reshape(nc, ROWS, 2 * XC).astype(BF16)
    for peer in col_peers:
        remote(t_out.at[peer], t_in.at[me_c], t_send, t_recv.at[me_c], "col", peer).start()

    others = c_in.at[pl.ds(0, (nf - 1) * XC)]
    remote(others, others, c_send, r_recv, "facet", me_f).wait_send()
    remote(others, others, r_send, r_recv, "facet", me_f).wait_send()

    total = dot(t_out[me_c], back[me_c])
    near_first = col_peers[::-1]
    cut = 3 * nc // 4
    for group in (near_first[:cut], near_first[cut:]):
        for peer in group:
            slot = t_in.at[peer]
            remote(slot, slot, t_send, t_recv.at[peer], "col", me_c).wait_recv()
        for peer in group:
            total += dot(t_in[peer], back[peer])
    total = total * (1.0 / math.sqrt(nc * nf))
    out_ref[pl.ds(0, ROWS, stride=2), :] = total[:, 0:SLAB]
    out_ref[pl.ds(1, ROWS, stride=2), :] = total[:, SLAB:]

    others = t_in.at[pl.ds(0, nc - 1)]
    remote(others, others, t_send, r_recv, "col", me_c).wait_send()


def body(nf, nc, facets, sub_offsets, col_offsets, screen_index, screens):
    block = 2 * ROWS
    height = ROWS * nc
    tables = fourier_tables(nf)
    hbm = pl.BlockSpec(memory_space=pltpu.HBM)
    in_hbm = functools.partial(pltpu.with_memory_space_constraint, memory_space=pltpu.HBM)
    smem = pl.BlockSpec(memory_space=pltpu.SMEM)
    vmem = pltpu.VMEM
    dma = pltpu.SemaphoreType.DMA
    out = pl.pallas_call(
        functools.partial(kernel, nf, nc),
        name="swiftly",
        out_shape=jax.ShapeDtypeStruct((block, SLAB), F32),
        in_specs=[hbm, hbm, smem, smem] + [hbm] * 5,
        out_specs=pl.BlockSpec(memory_space=pltpu.VMEM),
        scratch_shapes=[
            pltpu.SMEM((1, nf), jnp.int32),
            vmem(screens.shape, F32),
            *[vmem(t.shape, BF16) for t in tables],
            vmem((2 * height, SLAB), BF16),
            vmem((nf * XC, 2 * height), BF16),
            vmem((2 * height, nf * XC), BF16),
            vmem((SLAB, 2 * XC), BF16),
            vmem((nc, 1, SLAB), jnp.int32),
            vmem((nc, 2 * XC, 2 * SLAB), BF16),
            vmem((nf * XC, 2 * XC), BF16),
            vmem((nf * XC, 2 * XC), BF16),
            vmem((BLOCKS, SPAN, 2 * XC), F32),
            vmem((XS, 2 * XS), BF16),
            vmem((BLOCKS, SPAN, 2 * XC), F32),
            vmem((nf * XC, 2 * XC), BF16),
            vmem((nf * XC, 2 * XC), BF16),
            vmem((nc, ROWS, 2 * XC), BF16),
            vmem((nc, ROWS, 2 * XC), BF16),
            dma((7,)),
            dma,
            dma,
            dma,
            dma,
            dma,
            dma((nf,)),
            dma,
            dma,
            dma,
            dma((nc,)),
        ],
        compiler_params=pltpu.CompilerParams(collective_id=0, has_side_effects=True, vmem_limit_bytes=40 * 2**20),
    )(
        in_hbm(facets.reshape(block, SLAB)),
        in_hbm(sub_offsets),
        col_offsets,
        screen_index,
        in_hbm(screens),
        *map(in_hbm, tables),
    )
    return out.reshape(1, ROWS, 2, SLAB)


def solution(mesh):
    return jax.shard_map(
        functools.partial(body, mesh.shape["facet"], mesh.shape["col"]),
        mesh=mesh,
        in_specs=(P("facet", "col", None, None), P("col", None), P("col"), P("col", "facet"), P()),
        out_specs=P("facet", "col", None, None),
        check_vma=False,
    )
```

```python
import functools
import math

import jax
import jax.numpy as jnp
import numpy as np
from jax import lax
from jax.experimental import pallas as pl
from jax.experimental.pallas import tpu as pltpu
from jax.sharding import PartitionSpec as P

XC = 64
XS = 256
SLAB = 128
NPAD = 8192
STEP = 7
ROWS = 8
NEAR = 3
SPAN = 176
BLOCKS = 3
MESH = pl.DeviceIdType.MESH
F32 = jnp.float32
BF16 = jnp.bfloat16


def fourier_tables(facets):
    a = np.arange(XS)[:, None]
    q = np.arange(XS)[None, :]
    angle = 2.0 * np.pi * ((a * q) % XS) / XS
    keep = (q < STEP * (facets - 1) + XC).astype(np.float64)
    re = np.cos(angle) / math.sqrt(XS) * keep
    im = np.sin(angle) / math.sqrt(XS) * keep
    across = np.block([[re.T, im.T], [-im.T, re.T]])
    order = np.arange(BLOCKS * 2 * XC)
    order = order // (2 * XC) * XC + order % XC + order // XC % 2 * XS
    row_in = across[order]
    col_in = np.concatenate([re, im], axis=0) / math.sqrt(facets)
    col_out = np.concatenate([re.T[:SPAN], im.T[:SPAN]], axis=0)
    row_out = np.block([[re, -im], [im, re]])[:, order]
    return tuple(jnp.asarray(t, dtype=BF16) for t in (row_in, col_in, col_out, row_out))


def unit_circle(n):
    n = n & (NPAD - 1)
    quarter = (n + NPAD // 8) >> 11
    t = (n - (quarter << 11)).astype(F32) * (2.0 * math.pi / NPAD)
    t2 = t * t
    c = 1.0 + t2 * (-1.0 / 2 + t2 * (1.0 / 24 + t2 * (-1.0 / 720 + t2 * (1.0 / 40320))))
    s = t * (1.0 + t2 * (-1.0 / 6 + t2 * (1.0 / 120 + t2 * (-1.0 / 5040 + t2 * (1.0 / 362880)))))
    odd = (quarter & 1) == 1
    cos = jnp.where(odd, s, c)
    sin = jnp.where(odd, c, s)
    cos = jnp.where(((quarter + 1) & 2) == 2, -cos, cos)
    sin = jnp.where((quarter & 2) == 2, -sin, sin)
    return cos, sin


def iota(shape, dim):
    return lax.broadcasted_iota(jnp.int32, shape, dim)


def join_parts(t):
    rows = t.shape[0]
    even = (iota(t.shape, 0) & 1) == 0
    low = iota(t.shape, 1) < XC
    other = jnp.where(even, pltpu.roll(t, rows - 1, 0), pltpu.roll(t, 1, 0))
    other = pltpu.roll(other, XC, 1)
    return jnp.where(even == low, t - other, t + other)


def dot(a, b):
    return jnp.dot(a, b, preferred_element_type=F32)


def peers_of_col(me, count):
    ny = count // 4
    steps = [(dy, low) for dy in range(ny) for low in range(4) if dy or low]
    steps.sort(key=lambda k: -(min(k[0], ny - k[0]) + (k[1] >> 1)))
    y, rest = me >> 2, me & 3
    return [lax.rem(y + dy, ny) * 4 + (rest ^ low) for dy, low in steps]


def peers_of_facet(me, count):
    nz = count // 2
    steps = [(dx, dz) for dx in range(2) for dz in range(nz) if dx or dz]
    steps.sort(key=lambda k: (-k[0], -min(k[1], nz - k[1])))
    x, z = me // nz, lax.rem(me, nz)
    by_x = [(x ^ dx) * nz + lax.rem(z + dz, nz) for dx, dz in steps]
    steps.sort(key=lambda k: -(min(k[1], nz - k[1]) + 2 * k[0]))
    far = [(x ^ dx) * nz + lax.rem(z + dz, nz) for dx, dz in steps]
    near = [p for p, (dx, dz) in zip(far, steps) if min(dz, nz - dz) + 2 * dx <= NEAR]
    below = lax.rem(z + nz - 1, nz)
    return by_x, far, near, [(x ^ 1) * nz + z, (x ^ 1) * nz + below, x * nz + below]


def kernel(
    nf,
    nc,
    x_hbm,
    sub_hbm,
    col_s,
    idx_s,
    screens_hbm,
    row_in_hbm,
    col_in_hbm,
    col_out_hbm,
    row_out_hbm,
    out_ref,
    sub_s,
    screens,
    row_in,
    col_in,
    col_out,
    row_out,
    slab,
    phase,
    phase_t,
    across,
    offs,
    back,
    c_out,
    c_in,
    z,
    half,
    w,
    r_out,
    r_in,
    t_out,
    t_in,
    local_sem,
    ready,
    slab_send,
    slab_recv,
    offs_send,
    offs_recv,
    c_send,
    c_recv,
    r_send,
    r_recv,
    t_send,
    t_recv,
):
    me_f = lax.axis_index("facet")
    me_c = lax.axis_index("col")
    col_peers = peers_of_col(me_c, nc)
    facet_peers, facet_far, facet_near, told = peers_of_facet(me_f, nf)
    height = ROWS * nc
    block = 2 * ROWS

    def slab_rows(j):
        return pl.ds(pl.multiple_of(j * block, block), block)

    def sub_rows(s):
        return pl.ds(pl.multiple_of(s * XC, XC), XC)

    local = [
        pltpu.make_async_copy(src, dst, local_sem.at[i])
        for i, (src, dst) in enumerate(
            [
                (x_hbm, slab.at[slab_rows(me_c)]),
                (sub_hbm, sub_s),
                (screens_hbm, screens),
                (row_in_hbm, row_in),
                (col_in_hbm, col_in),
                (col_out_hbm, col_out),
                (row_out_hbm, row_out),
            ]
        )
    ]
    for copy in local:
        copy.start()

    offset = col_s[0]
    shift = STEP * me_f
    offs[me_c] = jnp.full((1, SLAB), offset, jnp.int32)

    barrier = pltpu.get_barrier_semaphore()

    for peer in col_peers:
        pl.semaphore_signal(barrier, 1, device_id={"col": peer}, device_id_type=MESH)
    for peer in facet_near:
        pl.semaphore_signal(barrier, 1, device_id={"facet": peer}, device_id_type=MESH)

    local[0].wait()
    pl.semaphore_wait(barrier, nc - 1 + len(facet_near))

    def remote(src, dst, send, recv, axis, peer):
        return pltpu.make_async_remote_copy(
            src_ref=src,
            dst_ref=dst,
            send_sem=send,
            recv_sem=recv,
            device_id={axis: peer},
            device_id_type=MESH,
        )

    mine = slab.at[slab_rows(me_c)]
    for peer in col_peers:
        remote(mine, mine, slab_send, slab_recv, "col", peer).start()
    for peer in told:
        pl.semaphore_signal(ready, 1, device_id={"facet": peer}, device_id_type=MESH)

    lane = iota((SLAB, 2 * XC), 1)
    cos, sin = unit_circle(iota((SLAB, 2 * XC), 0) * (offset + ((lane - shift) & (XC - 1))))
    across[...] = (jnp.where(lane < XC, cos, -sin) * (1.0 / math.sqrt(SLAB))).astype(BF16)

    local[1].wait()
    lane_row = (8, 2 * height)
    place = iota(lane_row, 1)
    row_id = me_f * height + (place >> 1)
    turn = (place & 1) * (NPAD // 4)
    within = iota((XC, 2 * height), 0)
    place_u = iota((XC, 2 * height), 1)
    cos_u, sin_u = unit_circle(within * (me_f * height + (place_u >> 1)))
    cos_u = cos_u.reshape(XC // 8, 8, 2 * height)
    sin_u = sin_u.reshape(XC // 8, 8, 2 * height)

    def fill_phase(s, carry):
        cos_s, sin_s = unit_circle(sub_s[0, s] * row_id - turn)
        scale = 1.0 / math.sqrt(height)
        values = (cos_s * scale)[None] * cos_u - (sin_s * scale)[None] * sin_u
        phase[sub_rows(s), :] = values.reshape(XC, 2 * height).astype(BF16)
        return carry

    lax.fori_loop(0, nf, fill_phase, 0)

    tall = (2 * height, 2 * XC)
    place_t = iota(tall, 0)
    second_t = place_t >= height
    row_t = me_f * height + jnp.where(second_t, place_t - height, place_t)
    turn_t = jnp.where(second_t, NPAD // 4, 0)
    lane_t = iota(tall, 1)

    def fill_phase_t(t, carry):
        freq = jnp.where(lane_t < XC, sub_s[0, 2 * t], sub_s[0, 2 * t + 1]) + (lane_t & (XC - 1))
        cos_t, _ = unit_circle(freq * row_t - turn_t)
        columns = pl.ds(pl.multiple_of(t * 2 * XC, 2 * XC), 2 * XC)
        phase_t[:, columns] = (cos_t * (1.0 / math.sqrt(height))).astype(BF16)
        return carry

    lax.fori_loop(0, nf // 2, fill_phase_t, 0)
    z[...] = jnp.zeros_like(z)
    half[...] = jnp.zeros_like(half)
    for copy in local[2:]:
        copy.wait()

    others = slab.at[pl.ds(0, (nc - 1) * block)]
    arrival = remote(others, others, slab_send, slab_recv, "col", me_c)
    arrival.wait_send()
    arrival.wait_recv()

    pl.semaphore_wait(ready, 3)
    spread = join_parts(dot(slab[...], across[...])).astype(BF16)
    half_rows = nf // 2 * XC
    far_half = (me_f // (nf // 2)) ^ 1
    for group in range(2):
        rows = pl.ds(pl.multiple_of((far_half ^ group) * half_rows, half_rows), half_rows)
        c_out[rows, :] = dot(phase[rows, :], spread).astype(BF16)
        for peer in facet_peers[nf // 2 * group : nf // 2 * (group + 1)]:
            remote(
                c_out.at[sub_rows(peer)],
                c_in.at[sub_rows(me_f)],
                c_send,
                c_recv.at[me_f],
                "facet",
                peer,
            ).start()
    c_in[sub_rows(me_f), :] = c_out[sub_rows(me_f), :]

    mine = offs.at[me_c]
    for peer in col_peers:
        remote(mine, mine, offs_send, offs_recv, "col", peer).start()

    others = offs.at[pl.ds(0, nc - 1)]
    arrival = remote(others, others, offs_send, offs_recv, "col", me_c)
    arrival.wait_send()
    arrival.wait_recv()
    at_x = iota((XC, SLAB), 1)
    at_v = (iota((XC, SLAB), 0) - shift) & (XC - 1)

    def fill_across(j, carry):
        cos_j, sin_j = unit_circle(at_x * (offs[j] + at_v))
        cos_j = cos_j * (1.0 / math.sqrt(SLAB))
        sin_j = sin_j * (1.0 / math.sqrt(SLAB))
        back[j, 0:XC, 0:SLAB] = cos_j.astype(BF16)
        back[j, 0:XC, SLAB:] = sin_j.astype(BF16)
        back[j, XC:, 0:SLAB] = (-sin_j).astype(BF16)
        back[j, XC:, SLAB:] = cos_j.astype(BF16)
        return carry

    lax.fori_loop(0, nc, fill_across, 0)

    lane_v = iota((XC, 2 * XC), 1) & (XC - 1)
    for f in range(nf):
        start = STEP * f
        first, inside = divmod(start, XC)
        rows = pl.ds(start, XC)

        @pl.when(f != me_f)
        def _():
            slot = c_in.at[pl.ds(f * XC, XC)]
            remote(slot, slot, c_send, c_recv.at[f], "facet", me_f).wait_recv()

        got = c_in[pl.ds(f * XC, XC), :].astype(F32)
        if inside:
            z[first, rows, :] += jnp.where(lane_v >= inside, got, 0.0)
            z[first + 1, rows, :] += jnp.where(lane_v >= inside, 0.0, got)
        else:
            z[first, rows, :] += got

    placed = jnp.concatenate([z[b].astype(BF16) for b in range(BLOCKS)], axis=1)
    half[0:SPAN, :] = dot(placed, row_in[...]).astype(BF16)
    grid = dot(col_in[...], half[...])
    sub_re = grid[0:XS, 0:XS] - grid[XS:, XS:]
    sub_im = grid[0:XS, XS:] + grid[XS:, 0:XS]
    g = idx_s[0, 0]
    gain_re = screens[g, 0]
    gain_im = screens[g, 1]
    screened = jnp.concatenate(
        [
            (sub_re * gain_re - sub_im * gain_im).astype(BF16),
            (sub_re * gain_im + sub_im * gain_re).astype(BF16),
        ],
        axis=1,
    )
    inner = dot(col_out[...], screened)
    inner = jnp.concatenate(
        [
            (inner[0:SPAN, 0:XS] + inner[SPAN:, XS:]).astype(BF16),
            (inner[0:SPAN, XS:] - inner[SPAN:, 0:XS]).astype(BF16),
        ],
        axis=1,
    )
    windows = dot(inner, row_out[...])
    for b in range(BLOCKS):
        w[b] = windows[:, b * 2 * XC : (b + 1) * 2 * XC]

    for f in range(nf):
        start = STEP * f
        first, inside = divmod(start, XC)
        rows = pl.ds(start, XC)
        cut = w[first, rows, :]
        if inside:
            cut = jnp.where(lane_v >= inside, cut, w[first + 1, rows, :])
        r_out[pl.ds(f * XC, XC), :] = cut.astype(BF16)

    for peer in facet_far:
        remote(
            r_out.at[sub_rows(peer)], r_in.at[sub_rows(me_f)], r_send, r_recv, "facet", peer
        ).start()
    r_in[sub_rows(me_f), :] = r_out[sub_rows(me_f), :]

    others = r_in.at[pl.ds(0, (nf - 1) * XC)]
    remote(others, others, r_send, r_recv, "facet", me_f).wait_recv()

    terms = dot(phase_t[...], r_in[...])
    turned = pltpu.roll(terms[height:], XC, 1)
    rows = terms[0:height] + jnp.where(iota((height, 2 * XC), 1) < XC, -turned, turned)
    t_out[...] = rows.reshape(nc, ROWS, 2 * XC).astype(BF16)
    for peer in col_peers:
        remote(t_out.at[peer], t_in.at[me_c], t_send, t_recv.at[me_c], "col", peer).start()

    others = c_in.at[pl.ds(0, (nf - 1) * XC)]
    remote(others, others, c_send, r_recv, "facet", me_f).wait_send()
    remote(others, others, r_send, r_recv, "facet", me_f).wait_send()

    total = dot(t_out[me_c], back[me_c])
    near_first = col_peers[::-1]
    cut = 3 * nc // 4
    for group in (near_first[:cut], near_first[cut:]):
        for peer in group:
            slot = t_in.at[peer]
            remote(slot, slot, t_send, t_recv.at[peer], "col", me_c).wait_recv()
        for peer in group:
            total += dot(t_in[peer], back[peer])
    total = total * (1.0 / math.sqrt(nc * nf))
    out_ref[pl.ds(0, ROWS, stride=2), :] = total[:, 0:SLAB]
    out_ref[pl.ds(1, ROWS, stride=2), :] = total[:, SLAB:]

    others = t_in.at[pl.ds(0, nc - 1)]
    remote(others, others, t_send, r_recv, "col", me_c).wait_send()


def body(nf, nc, facets, sub_offsets, col_offsets, screen_index, screens):
    block = 2 * ROWS
    height = ROWS * nc
    tables = fourier_tables(nf)
    hbm = pl.BlockSpec(memory_space=pltpu.HBM)
    in_hbm = functools.partial(pltpu.with_memory_space_constraint, memory_space=pltpu.HBM)
    smem = pl.BlockSpec(memory_space=pltpu.SMEM)
    vmem = pltpu.VMEM
    dma = pltpu.SemaphoreType.DMA
    out = pl.pallas_call(
        functools.partial(kernel, nf, nc),
        name="swiftly",
        out_shape=jax.ShapeDtypeStruct((block, SLAB), F32),
        in_specs=[hbm, hbm, smem, smem] + [hbm] * 5,
        out_specs=pl.BlockSpec(memory_space=pltpu.VMEM),
        scratch_shapes=[
            pltpu.SMEM((1, nf), jnp.int32),
            vmem(screens.shape, F32),
            *[vmem(t.shape, BF16) for t in tables],
            vmem((2 * height, SLAB), BF16),
            vmem((nf * XC, 2 * height), BF16),
            vmem((2 * height, nf * XC), BF16),
            vmem((SLAB, 2 * XC), BF16),
            vmem((nc, 1, SLAB), jnp.int32),
            vmem((nc, 2 * XC, 2 * SLAB), BF16),
            vmem((nf * XC, 2 * XC), BF16),
            vmem((nf * XC, 2 * XC), BF16),
            vmem((BLOCKS, SPAN, 2 * XC), F32),
            vmem((XS, 2 * XS), BF16),
            vmem((BLOCKS, SPAN, 2 * XC), F32),
            vmem((nf * XC, 2 * XC), BF16),
            vmem((nf * XC, 2 * XC), BF16),
            vmem((nc, ROWS, 2 * XC), BF16),
            vmem((nc, ROWS, 2 * XC), BF16),
            dma((7,)),
            pltpu.SemaphoreType.REGULAR,
            dma,
            dma,
            dma,
            dma,
            dma,
            dma((nf,)),
            dma,
            dma,
            dma,
            dma((nc,)),
        ],
        compiler_params=pltpu.CompilerParams(collective_id=0, has_side_effects=True, vmem_limit_bytes=40 * 2**20),
    )(
        in_hbm(facets.reshape(block, SLAB)),
        in_hbm(sub_offsets),
        col_offsets,
        screen_index,
        in_hbm(screens),
        *map(in_hbm, tables),
    )
    return out.reshape(1, ROWS, 2, SLAB)


def solution(mesh):
    return jax.shard_map(
        functools.partial(body, mesh.shape["facet"], mesh.shape["col"]),
        mesh=mesh,
        in_specs=(P("facet", "col", None, None), P("col", None), P("col"), P("col", "facet"), P()),
        out_specs=P("facet", "col", None, None),
        check_vma=False,
    )
```

```python
import functools
import math

import jax
import jax.numpy as jnp
import numpy as np
from jax import lax
from jax.experimental import pallas as pl
from jax.experimental.pallas import tpu as pltpu
from jax.sharding import PartitionSpec as P

XC = 64
XS = 256
SLAB = 128
NPAD = 8192
STEP = 7
ROWS = 8
NEAR = 3
SPAN = 176
BLOCKS = 3
MESH = pl.DeviceIdType.MESH
F32 = jnp.float32
BF16 = jnp.bfloat16


def fourier_tables(facets):
    a = np.arange(XS)[:, None]
    q = np.arange(XS)[None, :]
    angle = 2.0 * np.pi * ((a * q) % XS) / XS
    keep = (q < STEP * (facets - 1) + XC).astype(np.float64)
    re = np.cos(angle) / math.sqrt(XS) * keep
    im = np.sin(angle) / math.sqrt(XS) * keep
    across = np.block([[re.T, im.T], [-im.T, re.T]])
    order = np.arange(BLOCKS * 2 * XC)
    order = order // (2 * XC) * XC + order % XC + order // XC % 2 * XS
    row_in = across[order]
    col_in = np.concatenate([re, im], axis=0) / math.sqrt(facets)
    col_out = np.concatenate([re.T[:SPAN], im.T[:SPAN]], axis=0)
    row_out = np.block([[re, -im], [im, re]])[:, order]
    return tuple(jnp.asarray(t, dtype=BF16) for t in (row_in, col_in, col_out, row_out))


def unit_circle(n):
    n = n & (NPAD - 1)
    quarter = (n + NPAD // 8) >> 11
    t = (n - (quarter << 11)).astype(F32) * (2.0 * math.pi / NPAD)
    t2 = t * t
    c = 1.0 + t2 * (-1.0 / 2 + t2 * (1.0 / 24 + t2 * (-1.0 / 720 + t2 * (1.0 / 40320))))
    s = t * (1.0 + t2 * (-1.0 / 6 + t2 * (1.0 / 120 + t2 * (-1.0 / 5040 + t2 * (1.0 / 362880)))))
    odd = (quarter & 1) == 1
    cos = jnp.where(odd, s, c)
    sin = jnp.where(odd, c, s)
    cos = jnp.where(((quarter + 1) & 2) == 2, -cos, cos)
    sin = jnp.where((quarter & 2) == 2, -sin, sin)
    return cos, sin


def iota(shape, dim):
    return lax.broadcasted_iota(jnp.int32, shape, dim)


def join_parts(t):
    rows = t.shape[0]
    even = (iota(t.shape, 0) & 1) == 0
    low = iota(t.shape, 1) < XC
    other = jnp.where(even, pltpu.roll(t, rows - 1, 0), pltpu.roll(t, 1, 0))
    other = pltpu.roll(other, XC, 1)
    return jnp.where(even == low, t - other, t + other)


def dot(a, b):
    return jnp.dot(a, b, preferred_element_type=F32)


def peers_of_col(me, count):
    ny = count // 4
    steps = [(dy, low) for dy in range(ny) for low in range(4) if dy or low]
    steps.sort(key=lambda k: -(min(k[0], ny - k[0]) + (k[1] >> 1)))
    y, rest = me >> 2, me & 3
    return [lax.rem(y + dy, ny) * 4 + (rest ^ low) for dy, low in steps]


def peers_of_facet(me, count):
    nz = count // 2
    steps = [(dx, dz) for dx in range(2) for dz in range(nz) if dx or dz]
    steps.sort(key=lambda k: (-k[0], -min(k[1], nz - k[1])))
    x, z = me // nz, lax.rem(me, nz)
    by_x = [(x ^ dx) * nz + lax.rem(z + dz, nz) for dx, dz in steps]
    steps.sort(key=lambda k: -(min(k[1], nz - k[1]) + 2 * k[0]))
    far = [(x ^ dx) * nz + lax.rem(z + dz, nz) for dx, dz in steps]
    near = [p for p, (dx, dz) in zip(far, steps) if min(dz, nz - dz) + 2 * dx <= NEAR]
    below = lax.rem(z + nz - 1, nz)
    return by_x, far, near, [(x ^ 1) * nz + z, (x ^ 1) * nz + below, x * nz + below]


def kernel(
    nf,
    nc,
    x_hbm,
    sub_hbm,
    col_s,
    idx_s,
    screens_hbm,
    row_in_hbm,
    col_in_hbm,
    col_out_hbm,
    row_out_hbm,
    out_ref,
    sub_s,
    screens,
    row_in,
    col_in,
    col_out,
    row_out,
    slab,
    phase,
    phase_t,
    across,
    offs,
    back,
    c_out,
    c_in,
    z,
    half,
    w,
    r_out,
    r_in,
    t_out,
    t_in,
    local_sem,
    ready,
    slab_send,
    slab_recv,
    offs_send,
    offs_recv,
    c_send,
    c_recv,
    r_send,
    r_recv,
    t_send,
    t_recv,
):
    me_f = lax.axis_index("facet")
    me_c = lax.axis_index("col")
    col_peers = peers_of_col(me_c, nc)
    facet_peers, facet_far, facet_near, told = peers_of_facet(me_f, nf)
    height = ROWS * nc
    block = 2 * ROWS

    def slab_rows(j):
        return pl.ds(pl.multiple_of(j * block, block), block)

    def sub_rows(s):
        return pl.ds(pl.multiple_of(s * XC, XC), XC)

    local = [
        pltpu.make_async_copy(src, dst, local_sem.at[i])
        for i, (src, dst) in enumerate(
            [
                (x_hbm, slab.at[slab_rows(me_c)]),
                (sub_hbm, sub_s),
                (screens_hbm, screens),
                (row_in_hbm, row_in),
                (col_in_hbm, col_in),
                (col_out_hbm, col_out),
                (row_out_hbm, row_out),
            ]
        )
    ]
    for copy in local:
        copy.start()

    offset = col_s[0]
    shift = STEP * me_f
    offs[me_c] = jnp.full((1, SLAB), offset, jnp.int32)

    barrier = pltpu.get_barrier_semaphore()

    for peer in col_peers:
        pl.semaphore_signal(barrier, 1, device_id={"col": peer}, device_id_type=MESH)
    for peer in facet_near:
        pl.semaphore_signal(barrier, 1, device_id={"facet": peer}, device_id_type=MESH)

    local[0].wait()
    pl.semaphore_wait(barrier, nc - 1 + len(facet_near))

    def remote(src, dst, send, recv, axis, peer):
        return pltpu.make_async_remote_copy(
            src_ref=src,
            dst_ref=dst,
            send_sem=send,
            recv_sem=recv,
            device_id={axis: peer},
            device_id_type=MESH,
        )

    mine = slab.at[slab_rows(me_c)]
    for peer in col_peers:
        remote(mine, mine, slab_send, slab_recv, "col", peer).start()
    for peer in told:
        pl.semaphore_signal(ready, 1, device_id={"facet": peer}, device_id_type=MESH)

    lane = iota((SLAB, 2 * XC), 1)
    cos, sin = unit_circle(iota((SLAB, 2 * XC), 0) * (offset + ((lane - shift) & (XC - 1))))
    across[...] = (jnp.where(lane < XC, cos, -sin) * (1.0 / math.sqrt(SLAB))).astype(BF16)

    local[1].wait()
    lane_row = (8, 2 * height)
    place = iota(lane_row, 1)
    row_id = me_f * height + (place >> 1)
    turn = (place & 1) * (NPAD // 4)
    within = iota((XC, 2 * height), 0)
    place_u = iota((XC, 2 * height), 1)
    cos_u, sin_u = unit_circle(within * (me_f * height + (place_u >> 1)))
    cos_u = cos_u.reshape(XC // 8, 8, 2 * height)
    sin_u = sin_u.reshape(XC // 8, 8, 2 * height)

    def fill_phase(s, carry):
        cos_s, sin_s = unit_circle(sub_s[0, s] * row_id - turn)
        scale = 1.0 / math.sqrt(height)
        values = (cos_s * scale)[None] * cos_u - (sin_s * scale)[None] * sin_u
        phase[sub_rows(s), :] = values.reshape(XC, 2 * height).astype(BF16)
        return carry

    lax.fori_loop(0, nf, fill_phase, 0)

    tall = (2 * height, 2 * XC)
    place_t = iota(tall, 0)
    second_t = place_t >= height
    row_t = me_f * height + jnp.where(second_t, place_t - height, place_t)
    turn_t = jnp.where(second_t, NPAD // 4, 0)
    lane_t = iota(tall, 1)

    def fill_phase_t(t, carry):
        freq = jnp.where(lane_t < XC, sub_s[0, 2 * t], sub_s[0, 2 * t + 1]) + (lane_t & (XC - 1))
        cos_t, _ = unit_circle(freq * row_t - turn_t)
        columns = pl.ds(pl.multiple_of(t * 2 * XC, 2 * XC), 2 * XC)
        phase_t[:, columns] = (cos_t * (1.0 / math.sqrt(height))).astype(BF16)
        return carry

    lax.fori_loop(0, nf // 2, fill_phase_t, 0)
    z[...] = jnp.zeros_like(z)
    half[...] = jnp.zeros_like(half)
    for copy in local[2:]:
        copy.wait()

    others = slab.at[pl.ds(0, (nc - 1) * block)]
    arrival = remote(others, others, slab_send, slab_recv, "col", me_c)
    arrival.wait_send()
    arrival.wait_recv()

    pl.semaphore_wait(ready, 3)
    spread = join_parts(dot(slab[...], across[...])).astype(BF16)
    part = nf // 4
    part_rows = part * XC
    mine, inside = me_f // part, lax.rem(me_f, part)
    for group in range(4):
        first = (mine ^ (3 - group)) * part
        rows = pl.ds(pl.multiple_of(first * XC, part_rows), part_rows)
        c_out[rows, :] = dot(phase[rows, :], spread).astype(BF16)
        for step in range(1 if group == 3 else 0, part):
            peer = first + lax.rem(inside + step, part)
            remote(
                c_out.at[sub_rows(peer)],
                c_in.at[sub_rows(me_f)],
                c_send,
                c_recv.at[me_f],
                "facet",
                peer,
            ).start()
    c_in[sub_rows(me_f), :] = c_out[sub_rows(me_f), :]

    mine = offs.at[me_c]
    for peer in col_peers:
        remote(mine, mine, offs_send, offs_recv, "col", peer).start()

    others = offs.at[pl.ds(0, nc - 1)]
    arrival = remote(others, others, offs_send, offs_recv, "col", me_c)
    arrival.wait_send()
    arrival.wait_recv()
    at_x = iota((XC, SLAB), 1)
    at_v = (iota((XC, SLAB), 0) - shift) & (XC - 1)

    def fill_across(j, carry):
        cos_j, sin_j = unit_circle(at_x * (offs[j] + at_v))
        cos_j = cos_j * (1.0 / math.sqrt(SLAB))
        sin_j = sin_j * (1.0 / math.sqrt(SLAB))
        back[j, 0:XC, 0:SLAB] = cos_j.astype(BF16)
        back[j, 0:XC, SLAB:] = sin_j.astype(BF16)
        back[j, XC:, 0:SLAB] = (-sin_j).astype(BF16)
        back[j, XC:, SLAB:] = cos_j.astype(BF16)
        return carry

    lax.fori_loop(0, nc, fill_across, 0)

    lane_v = iota((XC, 2 * XC), 1) & (XC - 1)
    for f in range(nf):
        start = STEP * f
        first, inside = divmod(start, XC)
        rows = pl.ds(start, XC)

        @pl.when(f != me_f)
        def _():
            slot = c_in.at[pl.ds(f * XC, XC)]
            remote(slot, slot, c_send, c_recv.at[f], "facet", me_f).wait_recv()

        got = c_in[pl.ds(f * XC, XC), :].astype(F32)
        if inside:
            z[first, rows, :] += jnp.where(lane_v >= inside, got, 0.0)
            z[first + 1, rows, :] += jnp.where(lane_v >= inside, 0.0, got)
        else:
            z[first, rows, :] += got

    placed = jnp.concatenate([z[b].astype(BF16) for b in range(BLOCKS)], axis=1)
    half[0:SPAN, :] = dot(placed, row_in[...]).astype(BF16)
    grid = dot(col_in[...], half[...])
    sub_re = grid[0:XS, 0:XS] - grid[XS:, XS:]
    sub_im = grid[0:XS, XS:] + grid[XS:, 0:XS]
    g = idx_s[0, 0]
    gain_re = screens[g, 0]
    gain_im = screens[g, 1]
    screened = jnp.concatenate(
        [
            (sub_re * gain_re - sub_im * gain_im).astype(BF16),
            (sub_re * gain_im + sub_im * gain_re).astype(BF16),
        ],
        axis=1,
    )
    inner = dot(col_out[...], screened)
    inner = jnp.concatenate(
        [
            (inner[0:SPAN, 0:XS] + inner[SPAN:, XS:]).astype(BF16),
            (inner[0:SPAN, XS:] - inner[SPAN:, 0:XS]).astype(BF16),
        ],
        axis=1,
    )
    windows = dot(inner, row_out[...])
    for b in range(BLOCKS):
        w[b] = windows[:, b * 2 * XC : (b + 1) * 2 * XC]

    def cut_windows(low):
        for f in range(low, low + nf // 2):
            start = STEP * f
            block_q, inside_q = divmod(start, XC)
            rows_q = pl.ds(start, XC)
            piece = w[block_q, rows_q, :]
            if inside_q:
                piece = jnp.where(lane_v >= inside_q, piece, w[block_q + 1, rows_q, :])
            r_out[pl.ds(f * XC, XC), :] = piece.astype(BF16)

    for group in range(2):
        for half_x in range(2):

            @pl.when((me_f // (nf // 2)) ^ (1 - group) == half_x)
            def _():
                cut_windows(half_x * (nf // 2))

        for peer in facet_peers[nf // 2 * group : nf // 2 * (group + 1)]:
            remote(
                r_out.at[sub_rows(peer)], r_in.at[sub_rows(me_f)], r_send, r_recv, "facet", peer
            ).start()
    r_in[sub_rows(me_f), :] = r_out[sub_rows(me_f), :]

    others = r_in.at[pl.ds(0, (nf - 1) * XC)]
    remote(others, others, r_send, r_recv, "facet", me_f).wait_recv()

    terms = dot(phase_t[...], r_in[...])
    turned = pltpu.roll(terms[height:], XC, 1)
    rows = terms[0:height] + jnp.where(iota((height, 2 * XC), 1) < XC, -turned, turned)
    t_out[...] = rows.reshape(nc, ROWS, 2 * XC).astype(BF16)
    for peer in col_peers:
        remote(t_out.at[peer], t_in.at[me_c], t_send, t_recv.at[me_c], "col", peer).start()

    others = c_in.at[pl.ds(0, (nf - 1) * XC)]
    remote(others, others, c_send, r_recv, "facet", me_f).wait_send()
    remote(others, others, r_send, r_recv, "facet", me_f).wait_send()

    total = dot(t_out[me_c], back[me_c])
    near_first = col_peers[::-1]
    cut = 3 * nc // 4
    for group in (near_first[:cut], near_first[cut:]):
        for peer in group:
            slot = t_in.at[peer]
            remote(slot, slot, t_send, t_recv.at[peer], "col", me_c).wait_recv()
        for peer in group:
            total += dot(t_in[peer], back[peer])
    total = total * (1.0 / math.sqrt(nc * nf))
    out_ref[pl.ds(0, ROWS, stride=2), :] = total[:, 0:SLAB]
    out_ref[pl.ds(1, ROWS, stride=2), :] = total[:, SLAB:]

    others = t_in.at[pl.ds(0, nc - 1)]
    remote(others, others, t_send, r_recv, "col", me_c).wait_send()


def body(nf, nc, facets, sub_offsets, col_offsets, screen_index, screens):
    block = 2 * ROWS
    height = ROWS * nc
    tables = fourier_tables(nf)
    hbm = pl.BlockSpec(memory_space=pltpu.HBM)
    in_hbm = functools.partial(pltpu.with_memory_space_constraint, memory_space=pltpu.HBM)
    smem = pl.BlockSpec(memory_space=pltpu.SMEM)
    vmem = pltpu.VMEM
    dma = pltpu.SemaphoreType.DMA
    out = pl.pallas_call(
        functools.partial(kernel, nf, nc),
        name="swiftly",
        out_shape=jax.ShapeDtypeStruct((block, SLAB), F32),
        in_specs=[hbm, hbm, smem, smem] + [hbm] * 5,
        out_specs=pl.BlockSpec(memory_space=pltpu.VMEM),
        scratch_shapes=[
            pltpu.SMEM((1, nf), jnp.int32),
            vmem(screens.shape, F32),
            *[vmem(t.shape, BF16) for t in tables],
            vmem((2 * height, SLAB), BF16),
            vmem((nf * XC, 2 * height), BF16),
            vmem((2 * height, nf * XC), BF16),
            vmem((SLAB, 2 * XC), BF16),
            vmem((nc, 1, SLAB), jnp.int32),
            vmem((nc, 2 * XC, 2 * SLAB), BF16),
            vmem((nf * XC, 2 * XC), BF16),
            vmem((nf * XC, 2 * XC), BF16),
            vmem((BLOCKS, SPAN, 2 * XC), F32),
            vmem((XS, 2 * XS), BF16),
            vmem((BLOCKS, SPAN, 2 * XC), F32),
            vmem((nf * XC, 2 * XC), BF16),
            vmem((nf * XC, 2 * XC), BF16),
            vmem((nc, ROWS, 2 * XC), BF16),
            vmem((nc, ROWS, 2 * XC), BF16),
            dma((7,)),
            pltpu.SemaphoreType.REGULAR,
            dma,
            dma,
            dma,
            dma,
            dma,
            dma((nf,)),
            dma,
            dma,
            dma,
            dma((nc,)),
        ],
        compiler_params=pltpu.CompilerParams(collective_id=0, has_side_effects=True, vmem_limit_bytes=40 * 2**20),
    )(
        in_hbm(facets.reshape(block, SLAB)),
        in_hbm(sub_offsets),
        col_offsets,
        screen_index,
        in_hbm(screens),
        *map(in_hbm, tables),
    )
    return out.reshape(1, ROWS, 2, SLAB)


def solution(mesh):
    return jax.shard_map(
        functools.partial(body, mesh.shape["facet"], mesh.shape["col"]),
        mesh=mesh,
        in_specs=(P("facet", "col", None, None), P("col", None), P("col"), P("col", "facet"), P()),
        out_specs=P("facet", "col", None, None),
        check_vma=False,
    )
```
